256 devices in a mesh: row: 8 (over z_hi, core), col: 8 (over y, z_lo), dp: 4 (over x).
Axes of the slice: x: 4, y: 4, z: 8 (z_hi: 4, z_lo: 2; z = z_hi * 2 + z_lo), core: 2. Of those that a mesh axis runs over, the one named last changes fastest.
Arguments:
- inputs: bfloat16 [4096, 4096], P('dp', 'row'), may hold values from -6 to 6
- upstream: bfloat16 [4096, 4096], P('dp', 'row'), may hold values from -6 to 6
- expand: bfloat16 [4096, 16384], P('row', 'col'), may hold values from -0.09375 to 0.09375
- biases: float32 [16384], P('col'), may hold values from -5 to 5
- contract: bfloat16 [16384, 4096], P('col', 'row'), may hold values from -0.046875 to 0.046875
Outputs:
- grad_inputs: bfloat16 [4096, 4096], P('dp', 'row')
- grad_expand: bfloat16 [4096, 16384], P('row', 'col')
- grad_biases: bfloat16 [16384], P('col')
- grad_contract: bfloat16 [16384, 4096], P('col', 'row')
- grad_offset: bfloat16 [4096], P('row')
The draws below stay inside these ranges and needn't reach their ends.
All inputs are finite; a program needn't handle non-finite values.
Results may differ from the reference program's by a relative error of at most 0.022.
Values may be sent and summed in bfloat16 or wider, within the bound.
A program may use at most 128 MiB of HBM per device.

```python
import jax
import jax.numpy as jnp
from jax import lax

D = 4096
FF = 16384
TOK_DEV = 1024
TOKENS = 4096
N_ROW = 8
N_COL = 8
N_DP = 4


def levels(rng, extent, pieces, least, largest):
    level = 1.0
    for dim, parts in pieces:
        heights = jax.random.uniform(jax.random.fold_in(jax.random.fold_in(rng, 6), dim), (parts,), jnp.float32, least / len(pieces), largest / len(pieces))
        level = level * jnp.repeat(jnp.exp(heights), extent[dim] // parts).reshape((-1,) + (1,) * (len(extent) - 1 - dim))
    return level


def centred(own_key, dims, deviation, most, shards=(), kind=jnp.bfloat16):
    loudness = levels(own_key, dims, shards, -0.22, 0.18) if shards else 1.0
    entries = jax.random.normal(own_key, dims, jnp.float32) * deviation * loudness
    return jnp.minimum(jnp.maximum(entries, -most), most).astype(kind)


def setup_inputs(seed: int = 0) -> dict:
    splits = jax.random.split(jax.random.key(seed), 6)
    return {
        "inputs": centred(splits[0], (TOKENS, D), 1.0, 6.0, ((0, 4), (1, 8))),
        "upstream": centred(splits[1], (TOKENS, D), 1.0, 6.0, ((0, 4), (1, 8))),
        "expand": centred(splits[2], (D, FF), D ** -0.5, 0.09375, ((0, 8), (1, 8))),
        "biases": centred(splits[3], (FF,), 1.0, 5.0, ((0, 8),), jnp.float32),
        "contract": centred(splits[4], (FF, D), FF ** -0.5, 0.046875, ((0, 8), (1, 8))),
    }


def gelu_tanh(values):
    return jax.nn.gelu(values, approximate=True)

def rounded(values):
    return lax.optimization_barrier(values.astype(jnp.bfloat16)).astype(jnp.float32)

def reference(inputs, upstream, expand, biases, contract):
    width = D // N_ROW
    hidden_width = FF // N_COL
    pre_sum = jnp.zeros((TOKENS, FF), jnp.float32)
    back_sum = jnp.zeros((TOKENS, FF), jnp.float32)
    for index in range(N_ROW):
        first = index * width
        pre_part = jnp.dot(inputs[:, first:first + width], expand[first:first + width, :], preferred_element_type=jnp.float32)
        pre_sum = pre_sum + rounded(pre_part)
        back_part = jnp.dot(upstream[:, first:first + width], contract[:, first:first + width].T, preferred_element_type=jnp.float32)
        back_sum = back_sum + rounded(back_part)
    hidden = (pre_sum + biases[None, :]).astype(jnp.bfloat16)
    backward = back_sum.astype(jnp.bfloat16)
    forward_act, pullback = jax.vjp(gelu_tanh, hidden.astype(jnp.float32))
    slope_grad, = pullback(backward.astype(jnp.float32))
    activation = forward_act.astype(jnp.bfloat16)
    hidden_grad = slope_grad.astype(jnp.bfloat16)
    input_total = jnp.zeros((TOKENS, D), jnp.float32)
    for index in range(N_COL):
        first = index * hidden_width
        input_part = jnp.dot(hidden_grad[:, first:first + hidden_width], expand[:, first:first + hidden_width].T, preferred_element_type=jnp.float32)
        input_total = input_total + rounded(input_part)
    grad_inputs = input_total.astype(jnp.bfloat16)
    factor = TOKENS ** (-0.5)
    expand_total = jnp.zeros((D, FF), jnp.float32)
    biases_total = jnp.zeros((FF,), jnp.float32)
    contract_total = jnp.zeros((FF, D), jnp.float32)
    offset_total = jnp.zeros((D,), jnp.float32)
    for index in range(N_DP):
        first = index * TOK_DEV
        input_block = inputs[first:first + TOK_DEV]
        grad_block = hidden_grad[first:first + TOK_DEV]
        active_block = activation[first:first + TOK_DEV]
        upstream_block = upstream[first:first + TOK_DEV]
        expand_total = expand_total + rounded(jnp.dot(input_block.T, grad_block, preferred_element_type=jnp.float32) * factor)
        biases_total = biases_total + rounded(lax.optimization_barrier(jnp.sum(grad_block, axis=0, dtype=jnp.float32)) * factor)
        contract_total = contract_total + rounded(jnp.dot(active_block.T, upstream_block, preferred_element_type=jnp.float32) * factor)
        offset_total = offset_total + rounded(lax.optimization_barrier(jnp.sum(upstream_block, axis=0, dtype=jnp.float32)) * factor)
    return (grad_inputs, expand_total.astype(jnp.bfloat16), biases_total.astype(jnp.bfloat16), contract_total.astype(jnp.bfloat16), offset_total.astype(jnp.bfloat16))
```

```python
import functools

import jax
import jax.numpy as jnp
from jax import lax
from jax.experimental import pallas as pl
from jax.experimental.pallas import tpu as pltpu
from jax.sharding import PartitionSpec as P

BF = jnp.bfloat16
F32 = jnp.float32
MESH = pl.DeviceIdType.MESH
NN = (((1,), (0,)), ((), ()))
NT = (((1,), (1,)), ((), ()))
TN = (((0,), (0,)), ((), ()))


def dot(a, b, dims):
    return lax.dot_general(a, b, dims, preferred_element_type=F32)


class Net:
    def __init__(self, send_sem, recv_sem):
        self.send_sem, self.recv_sem = send_sem, recv_sem
        self.used, self.sent = 0, []

    def ids(self, count):
        first = self.used
        self.used += count
        return range(first, first + count)

    def send(self, k, src, dst, device):
        copy = pltpu.make_async_remote_copy(
            src, dst, self.send_sem.at[k], self.recv_sem.at[k], device_id=device, device_id_type=MESH
        )
        copy.start()
        self.sent.append(copy)

    def arrived(self, k, dst, device):
        pltpu.make_async_remote_copy(
            dst, dst, self.send_sem.at[k], self.recv_sem.at[k], device_id=device, device_id_type=MESH
        ).wait_recv()

    def drain(self):
        for copy in self.sent:
            copy.wait_send()


class Gather:
    def __init__(self, net, me, left, right, full, top, bottom):
        self.net, self.me, self.left, self.right = net, me, left, right
        self.full, self.top, self.bottom = full, top, bottom
        self.k = net.ids(4)

    def start(self):
        block = self.full(self.me)
        self.net.send(self.k[0], block, block, self.right)
        self.net.send(self.k[1], block, block, self.left)

    def forward(self):
        before, after = (self.me + 3) % 4, (self.me + 1) % 4
        self.net.arrived(self.k[0], self.full(before), self.left)
        self.net.send(self.k[2], self.top(before), self.top(before), self.right)
        self.net.arrived(self.k[1], self.full(after), self.right)
        self.net.send(self.k[3], self.bottom(after), self.bottom(after), self.left)

    def finish(self):
        across = (self.me + 2) % 4
        self.net.arrived(self.k[2], self.top(across), self.left)
        self.net.arrived(self.k[3], self.bottom(across), self.right)


class Exchange:
    def __init__(self, net, me, left, right, src, dst, relay, rows):
        self.net, self.me, self.left, self.right = net, me, left, right
        self.src, self.dst, self.relay, self.rows = src, dst, relay, rows
        self.k = net.ids(6)

    def start(self):
        me, half = self.me, self.rows // 2
        before, after, across = (me + 3) % 4, (me + 1) % 4, (me + 2) % 4
        self.net.send(self.k[2], self.src(across, 0, half), self.relay.at[0], self.right)
        self.net.send(self.k[3], self.src(across, half, half), self.relay.at[1], self.left)
        self.net.send(self.k[0], self.src(after, 0, self.rows), self.dst(me, 0, self.rows), self.right)
        self.net.send(self.k[1], self.src(before, 0, self.rows), self.dst(me, 0, self.rows), self.left)

    def forward(self):
        me, half = self.me, self.rows // 2
        before, after = (me + 3) % 4, (me + 1) % 4
        self.net.arrived(self.k[2], self.relay.at[0], self.left)
        self.net.send(self.k[4], self.relay.at[0], self.dst(before, 0, half), self.right)
        self.net.arrived(self.k[3], self.relay.at[1], self.right)
        self.net.send(self.k[5], self.relay.at[1], self.dst(after, half, half), self.left)

    def near(self):
        me = self.me
        self.net.arrived(self.k[0], self.dst((me + 3) % 4, 0, self.rows), self.left)
        self.net.arrived(self.k[1], self.dst((me + 1) % 4, 0, self.rows), self.right)

    def finish(self):
        half, across = self.rows // 2, (self.me + 2) % 4
        self.net.arrived(self.k[4], self.dst(across, 0, half), self.left)
        self.net.arrived(self.k[5], self.dst(across, half, half), self.right)


class Reduce:
    def __init__(self, net, me, left, right, part, inbox, add, total):
        self.net, self.me, self.left, self.right = net, me, left, right
        self.part, self.inbox, self.add, self.total = part, inbox, add, total
        self.k = net.ids(6)

    def far(self):
        across = (self.me + 2) % 4
        self.net.send(self.k[0], self.part(across, 0), self.inbox.at[0], self.right)
        self.net.send(self.k[1], self.part(across, 1), self.inbox.at[1], self.left)

    def near(self):
        before, after = (self.me + 3) % 4, (self.me + 1) % 4
        self.net.send(self.k[2], self.part(after, 1), self.inbox.at[2], self.right)
        self.net.send(self.k[3], self.part(before, 0), self.inbox.at[3], self.left)

    def join(self):
        before, after = (self.me + 3) % 4, (self.me + 1) % 4
        self.net.arrived(self.k[0], self.inbox.at[0], self.left)
        self.add(self.part(after, 0), self.inbox.at[0])
        self.net.send(self.k[4], self.part(after, 0), self.inbox.at[4], self.right)
        self.net.arrived(self.k[1], self.inbox.at[1], self.right)
        self.add(self.part(before, 1), self.inbox.at[1])
        self.net.send(self.k[5], self.part(before, 1), self.inbox.at[5], self.left)

    def finish(self):
        self.net.arrived(self.k[3], self.inbox.at[3], self.right)
        self.net.arrived(self.k[4], self.inbox.at[4], self.left)
        self.total(0, self.part(self.me, 0), self.inbox.at[3], self.inbox.at[4])
        self.net.arrived(self.k[2], self.inbox.at[2], self.left)
        self.net.arrived(self.k[5], self.inbox.at[5], self.right)
        self.total(1, self.part(self.me, 1), self.inbox.at[2], self.inbox.at[5])


def add_into(target, other):
    rows = 64
    lead = target.shape[0] if len(target.shape) == 3 else 1
    depth = target.shape[-2]

    def view(ref, i, r):
        where = pl.ds(pl.multiple_of(r * rows, rows), rows)
        return ref.at[i, where] if len(ref.shape) == 3 else ref.at[where]

    @pl.loop(0, lead * (depth // rows))
    def _(n):
        i, r = n // (depth // rows), n % (depth // rows)
        mine = view(target, i, r)
        mine[...] = (mine[...].astype(F32) + view(other, i, r)[...].astype(F32)).astype(BF)


def total_into(out, parts):
    rows = 64
    lead = out.shape[0] if len(out.shape) == 3 else 1
    depth = out.shape[-2]

    def view(ref, i, r):
        where = pl.ds(pl.multiple_of(r * rows, rows), rows)
        return ref.at[i, where] if len(ref.shape) == 3 else ref.at[where]

    @pl.loop(0, lead * (depth // rows))
    def _(n):
        i, r = n // (depth // rows), n % (depth // rows)
        acc = view(parts[0], i, r)[...].astype(F32)
        for other in parts[1:]:
            acc = acc + view(other, i, r)[...].astype(F32)
        view(out, i, r)[...] = acc.astype(BF)


def rows_at(start, size, unit):
    return pl.ds(pl.multiple_of(start, unit), size)


def kernel(
    x_ref, u_ref, e_ref, b_ref, c_ref,
    ox_ref, oe_ref, ob_ref, oc_ref, oo_ref,
    xg, ug, eg, cg, part, got, ah, relay_e, relay_c,
    ge, gc, gx, in_e, in_c, in_x, sum_e, sum_c, sum_x, relay_ge, relay_gc,
    pair_in, pair_sum, in_z, small, small_in,
    send_sem, recv_sem, local_sem, hid_send, hid_recv, act_send, act_recv,
):
    row, col, x = lax.axis_index("row"), lax.axis_index("col"), lax.axis_index("dp")
    zh, c = row // 2, row % 2
    y, zl = col // 2, col % 2
    factor = 1.0 / 64.0

    z_right, z_left = {"row": ((zh + 1) % 4) * 2 + c}, {"row": ((zh + 3) % 4) * 2 + c}
    z_across = {"row": ((zh + 2) % 4) * 2 + c}
    y_right, y_left = {"col": ((y + 1) % 4) * 2 + zl}, {"col": ((y + 3) % 4) * 2 + zl}
    x_right, x_left, x_across = {"dp": (x + 1) % 4}, {"dp": (x + 3) % 4}, {"dp": (x + 2) % 4}
    twin = {"row": zh * 2 + 1 - c}
    beside = {"col": y * 2 + 1 - zl}

    locals_ = [
        pltpu.make_async_copy(x_ref, xg.at[zh], local_sem.at[0]),
        pltpu.make_async_copy(u_ref, ug.at[zh], local_sem.at[1]),
        pltpu.make_async_copy(e_ref.at[:, rows_at(zh * 512, 512, 512)], eg.at[zh], local_sem.at[2]),
        pltpu.make_async_copy(c_ref.at[rows_at(zh * 512, 512, 512)], cg.at[zh], local_sem.at[3]),
    ]
    for copy in locals_:
        copy.start()

    barrier = pltpu.get_barrier_semaphore()
    peers = (z_right, z_left, z_across, y_right, y_left, x_right, x_left, x_across, twin, beside)
    for peer in peers:
        pl.semaphore_signal(barrier, inc=1, device_id=peer, device_id_type=MESH)
    pl.semaphore_wait(barrier, len(peers))

    net = Net(send_sem, recv_sem)

    def token_block(buf, d, size=256, first=0):
        return lambda j: buf.at[d, rows_at(j * 256 + first, size, 128)]

    def z_gather(buf):
        def at(size, first):
            return lambda j: buf.at[j, rows_at(y * 256 + first, size, 128)]
        return Gather(net, zh, z_left, z_right, at(256, 0), at(128, 0), at(128, 128))

    def y_gathers(buf):
        return [
            Gather(net, y, y_left, y_right, token_block(buf, (zh + d) % 4),
                   token_block(buf, (zh + d) % 4, 128), token_block(buf, (zh + d) % 4, 128, 128))
            for d in (1, 2, 3)
        ]

    def x_gathers(buf):
        def at(d, size, first):
            return lambda j: buf.at[(zh + d) % 4, rows_at(j * 128 + first, size, 64)]
        return [
            Gather(net, x, x_left, x_right, at(d, 128, 0), at(d, 64, 0), at(d, 64, 64))
            for d in (1, 2, 3)
        ]

    def weight_slot(buf):
        return lambda j, first, size: buf.at[j, rows_at(x * 128 + first, size, 64)]

    xz, uz = z_gather(xg), z_gather(ug)
    xy, uy = y_gathers(xg), y_gathers(ug)
    ez = Exchange(
        net, zh, z_left, z_right,
        lambda j, first, size: e_ref.at[rows_at(x * 128 + first, size, 64), rows_at(j * 512, 512, 512)],
        weight_slot(eg), relay_e, 128,
    )
    cz = Exchange(
        net, zh, z_left, z_right,
        lambda j, first, size: c_ref.at[rows_at(j * 512 + x * 128 + first, size, 64)],
        weight_slot(cg), relay_c, 128,
    )
    ex, cx = x_gathers(eg), x_gathers(cg)

    locals_[0].wait()
    xz.start()
    ez.start()
    locals_[1].wait()
    xz.forward()
    xy[0].start()
    xy[2].start()
    uz.start()
    ez.forward()
    ez.near()
    ex[0].start()
    ex[2].start()
    cz.start()
    xy[0].forward()
    xy[2].forward()
    xz.finish()
    xy[1].start()
    ez.finish()
    ex[1].start()
    uz.forward()
    uy[0].start()
    uy[2].start()
    ex[0].forward()
    ex[2].forward()
    cz.forward()
    cz.near()
    cx[0].start()
    cx[2].start()
    xy[1].forward()
    ex[1].forward()
    uz.finish()
    uy[1].start()
    cz.finish()
    cx[1].start()
    uy[0].forward()
    uy[2].forward()
    cx[0].forward()
    cx[2].forward()
    cx[1].forward()
    uy[1].forward()
    locals_[2].wait()
    locals_[3].wait()
    for group in (ex, xy, cx, uy):
        for gather in group:
            gather.finish()

    def hid_copy(k, slot):
        return pltpu.make_async_remote_copy(
            part.at[k, slot, 1 - c], got.at[k, slot], hid_send.at[k, slot], hid_recv.at[k, slot],
            device_id=twin, device_id_type=MESH,
        )

    def act_copy(k, slot):
        block = ah.at[k, c, rows_at(slot * 256, 256, 256)]
        return pltpu.make_async_remote_copy(
            block, block, act_send.at[k, slot], act_recv.at[k, slot],
            device_id=twin, device_id_type=MESH,
        )

    def act_landing(k, slot):
        block = ah.at[k, 1 - c, rows_at(slot * 256, 256, 256)]
        return pltpu.make_async_remote_copy(
            block, block, act_send.at[k, slot], act_recv.at[k, slot],
            device_id=twin, device_id_type=MESH,
        )

    @pl.loop(0, 4)
    def _(slot):
        where = rows_at(slot * 256, 256, 256)
        for half in range(2):
            cols = pl.ds(half * 256, 256)
            acc = dot(xg[0, where], eg[0, :, cols], NN)
            for j in range(1, 4):
                acc = acc + dot(xg[j, where], eg[j, :, cols], NN)
            part[0, slot, half] = acc
            acc = dot(ug[0, where], cg[0, cols], NT)
            for j in range(1, 4):
                acc = acc + dot(ug[j, where], cg[j, cols], NT)
            part[1, slot, half] = acc
        hid_copy(0, slot).start()
        hid_copy(1, slot).start()

    @pl.loop(0, 4)
    def _(slot):
        hid_copy(0, slot).wait_recv()
        hid_copy(1, slot).wait_recv()
        bias = b_ref[row]

        @pl.loop(0, 8)
        def _(r):
            rows = rows_at(r * 32, 32, 32)
            pre = part[0, slot, c, rows] + got[0, slot, rows] + bias
            v = pre.astype(BF).astype(F32)
            back = (part[1, slot, c, rows] + got[1, slot, rows]).astype(BF).astype(F32)
            k0, k1 = 0.7978845608028654, 0.044715
            sq = v * v
            t = jnp.tanh(k0 * (v + k1 * (sq * v)))
            half = 0.5 * (1.0 + t)
            slope = half + (0.5 * v) * (1.0 - t * t) * (k0 * (1.0 + 3.0 * k1 * sq))
            out = rows_at(slot * 256 + r * 32, 32, 32)
            ah[0, c, out] = (v * half).astype(BF)
            ah[1, c, out] = (back * slope).astype(BF)

        act_copy(0, slot).start()
        act_copy(1, slot).start()

    @pl.loop(0, 4)
    def _(slot):
        for k in range(2):
            act_landing(k, slot).wait_recv()
            hid_copy(k, slot).wait_send()
            act_copy(k, slot).wait_send()

    e_red = Reduce(
        net, x, x_left, x_right, lambda j, h: ge.at[j, pl.ds(2 * h, 2)], in_e, add_into,
        lambda h, *parts: total_into(sum_e.at[pl.ds(2 * h, 2)], parts),
    )
    c_red = Reduce(
        net, x, x_left, x_right, lambda j, h: gc.at[j, pl.ds(2 * h, 2)], in_c, add_into,
        lambda h, *parts: total_into(sum_c.at[pl.ds(2 * h, 2)], parts),
    )
    x_red = Reduce(
        net, y, y_left, y_right, lambda j, h: gx.at[j, pl.ds(2 * h, 2)], in_x, add_into,
        lambda h, *parts: total_into(sum_x.at[pl.ds(2 * h, 2)], parts),
    )
    own_rows = ox_ref.at[col]
    z_red = Reduce(
        net, zh, z_left, z_right, lambda j, h: pair_sum.at[j, pl.ds(64 * h, 64)], in_z, add_into,
        lambda h, *parts: total_into(own_rows.at[pl.ds(64 * h, 64)], parts),
    )
    e_swap = Exchange(
        net, zh, z_left, z_right, lambda j, first, size: sum_e.at[j, pl.ds(first, size)],
        lambda j, first, size: oe_ref.at[x, j, pl.ds(first, size)], relay_ge, 128,
    )
    c_swap = Exchange(
        net, zh, z_left, z_right, lambda j, first, size: sum_c.at[j, pl.ds(first, size)],
        lambda j, first, size: oc_ref.at[x, j, pl.ds(first, size)], relay_gc, 128,
    )

    def out_gather(ref):
        return Gather(
            net, x, x_left, x_right, lambda j: ref.at[j],
            lambda j: ref.at[j, pl.ds(0, 2)], lambda j: ref.at[j, pl.ds(2, 2)],
        )

    e_out, c_out = out_gather(oe_ref), out_gather(oc_ref)
    x_out = Gather(
        net, y, y_left, y_right, lambda j: ox_ref.at[pl.ds(2 * j, 2)],
        lambda j: ox_ref.at[2 * j], lambda j: ox_ref.at[2 * j + 1],
    )

    @pl.loop(0, 4)
    def _(j):
        for h in range(2):
            acc = (dot(xg[j], ah[1, h], TN) * factor).astype(BF)
            for q in range(4):
                ge[q, j, :, pl.ds(h * 256, 256)] = acc[q * 128:(q + 1) * 128]

    e_red.far()
    e_red.near()

    @pl.loop(0, 4)
    def _(j):
        for h in range(2):
            acc = (dot(ah[0, h], ug[j], TN) * factor).astype(BF)
            gc[2 * h, j] = acc[:128]
            gc[2 * h + 1, j] = acc[128:]

    c_red.far()

    @pl.loop(0, 4)
    def _(slot):
        where = rows_at(slot * 256, 256, 256)
        for j in range(4):
            acc = dot(ah[1, 0, where], eg[j, :, pl.ds(0, 256)], NT)
            acc = acc + dot(ah[1, 1, where], eg[j, :, pl.ds(256, 256)], NT)
            gx[slot, j] = acc.astype(BF)

    x_red.far()
    x_red.near()
    e_red.join()
    c_red.near()

    for h in range(2):
        def add_rows(n, acc):
            block = ah[1, h, rows_at(n * 64, 64, 64)].astype(F32)
            return acc + jnp.sum(block.reshape(8, 8, 256), axis=0)
        acc = lax.fori_loop(0, 16, add_rows, jnp.zeros((8, 256), F32))
        acc = jnp.sum(acc, axis=0, keepdims=True) * factor
        small[pl.ds(0, 8), pl.ds(h * 256, 256)] = jnp.broadcast_to(acc.astype(BF).astype(F32), (8, 256))

    def add_up(n, acc):
        block = ug[zh, rows_at(n * 64, 64, 64)].astype(F32)
        return acc + jnp.sum(block.reshape(8, 8, 512), axis=0)
    acc = lax.fori_loop(0, 16, add_up, jnp.zeros((8, 512), F32))
    acc = jnp.sum(acc, axis=0, keepdims=True) * factor
    small[pl.ds(8, 8)] = jnp.broadcast_to(acc.astype(BF).astype(F32), (8, 512))
    small_k = net.ids(6)
    for n, peer in enumerate((x_right, x_left, x_across)):
        net.send(small_k[n], small, small_in.at[n], peer)

    c_red.join()
    x_red.join()
    for n, peer in enumerate((x_left, x_right, x_across)):
        net.arrived(small_k[n], small_in.at[n], peer)
    whole = ((small[...] + small_in[0]) + small_in[1]) + small_in[2]
    ob_ref[zh] = whole[:8]
    oo_ref[...] = whole[8:]
    for n, peer in enumerate((z_right, z_left, z_across)):
        net.send(small_k[3 + n], ob_ref.at[zh], ob_ref.at[zh], peer)

    e_red.finish()
    oe_ref[x, zh] = sum_e[zh]
    e_swap.start()
    c_red.finish()
    oc_ref[x, zh] = sum_c[zh]
    e_swap.forward()
    c_swap.start()
    e_swap.near()
    e_swap.finish()
    e_out.start()
    x_red.finish()
    pair_k = net.ids(2)
    net.send(pair_k[0], sum_x.at[:, rows_at((1 - zl) * 128, 128, 128)], pair_in, beside)
    c_swap.forward()
    c_swap.near()
    c_swap.finish()
    c_out.start()
    net.arrived(pair_k[0], pair_in, beside)

    @pl.loop(0, 4)
    def _(j):
        mine = sum_x[j, rows_at(zl * 128, 128, 128)].astype(F32)
        pair_sum[j] = (mine + pair_in[j].astype(F32)).astype(BF)

    z_red.far()
    z_red.near()
    z_red.join()
    e_out.forward()
    z_red.finish()
    net.send(pair_k[1], own_rows, own_rows, beside)
    net.arrived(pair_k[1], ox_ref.at[y * 2 + 1 - zl], beside)
    x_out.start()
    c_out.forward()
    x_out.forward()
    e_out.finish()
    x_out.finish()
    c_out.finish()
    for n, d in enumerate((3, 1, 2)):
        net.arrived(small_k[3 + n], ob_ref.at[(zh + d) % 4], z_across)
    net.drain()
    assert net.used <= 160


def local(inputs, upstream, expand, biases, contract):
    vmem = pl.BlockSpec(memory_space=pltpu.VMEM)
    anywhere = pl.BlockSpec(memory_space=pl.ANY)
    dma = pltpu.SemaphoreType.DMA
    ox, oe, ob, oc, oo = pl.pallas_call(
        kernel,
        out_shape=(
            jax.ShapeDtypeStruct((8, 128, 512), BF),
            jax.ShapeDtypeStruct((4, 4, 128, 512), BF),
            jax.ShapeDtypeStruct((4, 8, 512), F32),
            jax.ShapeDtypeStruct((4, 4, 128, 512), BF),
            jax.ShapeDtypeStruct((8, 512), F32),
        ),
        in_specs=[anywhere, anywhere, anywhere, vmem, anywhere],
        out_specs=(vmem, vmem, vmem, vmem, vmem),
        scratch_shapes=[
            pltpu.VMEM((4, 1024, 512), BF),
            pltpu.VMEM((4, 1024, 512), BF),
            pltpu.VMEM((4, 512, 512), BF),
            pltpu.VMEM((4, 512, 512), BF),
            pltpu.VMEM((2, 4, 2, 256, 256), F32),
            pltpu.VMEM((2, 4, 256, 256), F32),
            pltpu.VMEM((2, 2, 1024, 256), BF),
            pltpu.VMEM((2, 64, 512), BF),
            pltpu.VMEM((2, 64, 512), BF),
            pltpu.VMEM((4, 4, 128, 512), BF),
            pltpu.VMEM((4, 4, 128, 512), BF),
            pltpu.VMEM((4, 4, 256, 512), BF),
            pltpu.VMEM((6, 2, 128, 512), BF),
            pltpu.VMEM((6, 2, 128, 512), BF),
            pltpu.VMEM((6, 2, 256, 512), BF),
            pltpu.VMEM((4, 128, 512), BF),
            pltpu.VMEM((4, 128, 512), BF),
            pltpu.VMEM((4, 256, 512), BF),
            pltpu.VMEM((2, 64, 512), BF),
            pltpu.VMEM((2, 64, 512), BF),
            pltpu.VMEM((4, 128, 512), BF),
            pltpu.VMEM((4, 128, 512), BF),
            pltpu.VMEM((6, 64, 512), BF),
            pltpu.VMEM((16, 512), F32),
            pltpu.VMEM((3, 16, 512), F32),
            dma((160,)),
            dma((160,)),
            dma((4,)),
            dma((2, 4)),
            dma((2, 4)),
            dma((2, 4)),
            dma((2, 4)),
        ],
        compiler_params=pltpu.CompilerParams(
            collective_id=0, has_side_effects=True, vmem_limit_bytes=60 * 1024 * 1024
        ),
    )(inputs, upstream, expand, biases.reshape(8, 1, 256), contract)
    return (
        ox.reshape(1024, 512),
        oe.transpose(0, 2, 1, 3).reshape(512, 2048),
        ob[:, 0, :].reshape(2048).astype(BF),
        oc.transpose(1, 0, 2, 3).reshape(2048, 512),
        oo[0].astype(BF),
    )


def solution(mesh):
    in_specs = (P("dp", "row"), P("dp", "row"), P("row", "col"), P("col"), P("col", "row"))
    out_specs = (P("dp", "row"), P("row", "col"), P("col"), P("col", "row"), P("row"))
    return jax.shard_map(local, mesh=mesh, in_specs=in_specs, out_specs=out_specs, check_vma=False)
```

```python
import functools

import jax
import jax.numpy as jnp
from jax import lax
from jax.experimental import pallas as pl
from jax.experimental.pallas import tpu as pltpu
from jax.sharding import PartitionSpec as P

BF = jnp.bfloat16
F32 = jnp.float32
MESH = pl.DeviceIdType.MESH
NN = (((1,), (0,)), ((), ()))
NT = (((1,), (1,)), ((), ()))
TN = (((0,), (0,)), ((), ()))


def dot(a, b, dims):
    return lax.dot_general(a, b, dims, preferred_element_type=F32)


class Net:
    def __init__(self, send_sem, recv_sem):
        self.send_sem, self.recv_sem = send_sem, recv_sem
        self.used, self.sent = 0, []

    def ids(self, count):
        first = self.used
        self.used += count
        return range(first, first + count)

    def send(self, k, src, dst, device):
        copy = pltpu.make_async_remote_copy(
            src, dst, self.send_sem.at[k], self.recv_sem.at[k], device_id=device, device_id_type=MESH
        )
        copy.start()
        self.sent.append(copy)

    def arrived(self, k, dst, device):
        pltpu.make_async_remote_copy(
            dst, dst, self.send_sem.at[k], self.recv_sem.at[k], device_id=device, device_id_type=MESH
        ).wait_recv()

    def drain(self):
        for copy in self.sent:
            copy.wait_send()


class Gather:
    def __init__(self, net, me, left, right, full, top, bottom):
        self.net, self.me, self.left, self.right = net, me, left, right
        self.full, self.top, self.bottom = full, top, bottom
        self.k = net.ids(4)

    def start(self):
        block = self.full(self.me)
        self.net.send(self.k[0], block, block, self.right)
        self.net.send(self.k[1], block, block, self.left)

    def forward(self):
        before, after = (self.me + 3) % 4, (self.me + 1) % 4
        self.net.arrived(self.k[0], self.full(before), self.left)
        self.net.send(self.k[2], self.top(before), self.top(before), self.right)
        self.net.arrived(self.k[1], self.full(after), self.right)
        self.net.send(self.k[3], self.bottom(after), self.bottom(after), self.left)

    def finish(self):
        across = (self.me + 2) % 4
        self.net.arrived(self.k[2], self.top(across), self.left)
        self.net.arrived(self.k[3], self.bottom(across), self.right)


class Exchange:
    def __init__(self, net, me, left, right, src, dst, relay, rows):
        self.net, self.me, self.left, self.right = net, me, left, right
        self.src, self.dst, self.relay, self.rows = src, dst, relay, rows
        self.k = net.ids(6)

    def start(self):
        me, half = self.me, self.rows // 2
        before, after, across = (me + 3) % 4, (me + 1) % 4, (me + 2) % 4
        self.net.send(self.k[2], self.src(across, 0, half), self.relay.at[0], self.right)
        self.net.send(self.k[3], self.src(across, half, half), self.relay.at[1], self.left)
        self.net.send(self.k[0], self.src(after, 0, self.rows), self.dst(me, 0, self.rows), self.right)
        self.net.send(self.k[1], self.src(before, 0, self.rows), self.dst(me, 0, self.rows), self.left)

    def forward(self):
        me, half = self.me, self.rows // 2
        before, after = (me + 3) % 4, (me + 1) % 4
        self.net.arrived(self.k[2], self.relay.at[0], self.left)
        self.net.send(self.k[4], self.relay.at[0], self.dst(before, 0, half), self.right)
        self.net.arrived(self.k[3], self.relay.at[1], self.right)
        self.net.send(self.k[5], self.relay.at[1], self.dst(after, half, half), self.left)

    def near(self):
        me = self.me
        self.net.arrived(self.k[0], self.dst((me + 3) % 4, 0, self.rows), self.left)
        self.net.arrived(self.k[1], self.dst((me + 1) % 4, 0, self.rows), self.right)

    def finish(self):
        half, across = self.rows // 2, (self.me + 2) % 4
        self.net.arrived(self.k[4], self.dst(across, 0, half), self.left)
        self.net.arrived(self.k[5], self.dst(across, half, half), self.right)


class Reduce:
    def __init__(self, net, me, left, right, part, inbox, add, total):
        self.net, self.me, self.left, self.right = net, me, left, right
        self.part, self.inbox, self.add, self.total = part, inbox, add, total
        self.k = net.ids(6)

    def far(self):
        across = (self.me + 2) % 4
        self.net.send(self.k[0], self.part(across, 0), self.inbox.at[0], self.right)
        self.net.send(self.k[1], self.part(across, 1), self.inbox.at[1], self.left)

    def near(self):
        before, after = (self.me + 3) % 4, (self.me + 1) % 4
        self.net.send(self.k[2], self.part(after, 1), self.inbox.at[2], self.right)
        self.net.send(self.k[3], self.part(before, 0), self.inbox.at[3], self.left)

    def join(self):
        before, after = (self.me + 3) % 4, (self.me + 1) % 4
        self.net.arrived(self.k[0], self.inbox.at[0], self.left)
        self.add(self.part(after, 0), self.inbox.at[0])
        self.net.send(self.k[4], self.part(after, 0), self.inbox.at[4], self.right)
        self.net.arrived(self.k[1], self.inbox.at[1], self.right)
        self.add(self.part(before, 1), self.inbox.at[1])
        self.net.send(self.k[5], self.part(before, 1), self.inbox.at[5], self.left)

    def finish(self):
        self.net.arrived(self.k[3], self.inbox.at[3], self.right)
        self.net.arrived(self.k[4], self.inbox.at[4], self.left)
        self.total(0, self.part(self.me, 0), self.inbox.at[3], self.inbox.at[4])
        self.net.arrived(self.k[2], self.inbox.at[2], self.left)
        self.net.arrived(self.k[5], self.inbox.at[5], self.right)
        self.total(1, self.part(self.me, 1), self.inbox.at[2], self.inbox.at[5])


def add_into(target, other):
    rows = min(64, target.shape[-2])
    lead = target.shape[0] if len(target.shape) == 3 else 1
    depth = target.shape[-2]

    def view(ref, i, r):
        where = pl.ds(pl.multiple_of(r * rows, rows), rows)
        return ref.at[i, where] if len(ref.shape) == 3 else ref.at[where]

    @pl.loop(0, lead * (depth // rows))
    def _(n):
        i, r = n // (depth // rows), n % (depth // rows)
        mine = view(target, i, r)
        mine[...] = (mine[...].astype(F32) + view(other, i, r)[...].astype(F32)).astype(BF)


def total_into(out, parts):
    rows = min(64, out.shape[-2])
    lead = out.shape[0] if len(out.shape) == 3 else 1
    depth = out.shape[-2]

    def view(ref, i, r):
        where = pl.ds(pl.multiple_of(r * rows, rows), rows)
        return ref.at[i, where] if len(ref.shape) == 3 else ref.at[where]

    @pl.loop(0, lead * (depth // rows))
    def _(n):
        i, r = n // (depth // rows), n % (depth // rows)
        acc = view(parts[0], i, r)[...].astype(F32)
        for other in parts[1:]:
            acc = acc + view(other, i, r)[...].astype(F32)
        view(out, i, r)[...] = acc.astype(BF)


def rows_at(start, size, unit):
    return pl.ds(pl.multiple_of(start, unit), size)


class PairRing:
    def __init__(self, net, zh, zl, outer, inner, block):
        self.net, self.outer, self.inner, self.block = net, outer, inner, block
        self.own, self.across = zh, (zh + 2) % 4
        self.early, self.late = (zh + 3 + 2 * zl) % 4, (zh + 5 - 2 * zl) % 4
        self.out_half, self.in_half = (1 - zl) * 128, zl * 128
        self.k = net.ids(4)

    def send(self, k, block, device):
        self.net.send(self.k[k], block, block, device)

    def start(self):
        self.send(0, self.block(self.own, 0, 256), self.outer)

    def get_early(self):
        block = self.block(self.early, 0, 256)
        self.net.arrived(self.k[0], block, self.outer)
        self.send(1, block, self.inner)

    def get_late(self):
        self.net.arrived(self.k[1], self.block(self.late, 0, 256), self.inner)
        self.send(2, self.block(self.late, self.out_half, 128), self.outer)

    def get_across(self):
        block = self.block(self.across, self.in_half, 128)
        self.net.arrived(self.k[2], block, self.outer)
        self.send(3, block, self.inner)

    def finish(self):
        self.net.arrived(self.k[3], self.block(self.across, self.out_half, 128), self.inner)


def kernel(
    x_ref, u_ref, e_ref, b_ref, c_ref,
    ox_ref, oe_ref, ob_ref, oc_ref, oo_ref,
    xg, ug, eg, cg, part, got, ah, relay_e, relay_c,
    ge, gc, gx, in_e, in_c, in_x, sum_e, sum_c, sum_x, relay_ge, relay_gc,
    pair_in, pair_sum, in_z, small, small_in,
    send_sem, recv_sem, local_sem, hid_send, hid_recv, act_send, act_recv,
):
    row, col, x = lax.axis_index("row"), lax.axis_index("col"), lax.axis_index("dp")
    zh, c = row // 2, row % 2
    y, zl = col // 2, col % 2
    factor = 1.0 / 64.0

    z_right, z_left = {"row": ((zh + 1) % 4) * 2 + c}, {"row": ((zh + 3) % 4) * 2 + c}
    z_across = {"row": ((zh + 2) % 4) * 2 + c}
    y_right, y_left = {"col": ((y + 1) % 4) * 2 + zl}, {"col": ((y + 3) % 4) * 2 + zl}
    x_right, x_left, x_across = {"dp": (x + 1) % 4}, {"dp": (x + 3) % 4}, {"dp": (x + 2) % 4}
    twin = {"row": zh * 2 + 1 - c}
    beside = {"col": y * 2 + 1 - zl}
    outer = {"row": ((zh + 3 + 2 * zl) % 4) * 2 + c, "col": y * 2 + 1 - zl}

    locals_ = [
        pltpu.make_async_copy(x_ref, xg.at[zh], local_sem.at[0]),
        pltpu.make_async_copy(u_ref, ug.at[zh], local_sem.at[1]),
        pltpu.make_async_copy(e_ref.at[:, rows_at(zh * 512, 512, 512)], eg.at[zh], local_sem.at[2]),
        pltpu.make_async_copy(c_ref.at[rows_at(zh * 512, 512, 512)], cg.at[zh], local_sem.at[3]),
    ]
    for copy in locals_:
        copy.start()

    barrier = pltpu.get_barrier_semaphore()
    peers = (z_right, z_left, z_across, y_right, y_left, x_right, x_left, x_across, twin, beside, outer)
    for peer in peers:
        pl.semaphore_signal(barrier, inc=1, device_id=peer, device_id_type=MESH)
    pl.semaphore_wait(barrier, len(peers))

    net = Net(send_sem, recv_sem)

    def z_gather(buf):
        return PairRing(
            net, zh, zl, outer, beside, lambda j, first, size: buf.at[j, rows_at(y * 256 + first, size, 128)]
        )

    def y_gathers(buf, ring):
        def gather(d):
            def at(size, first):
                return lambda j: buf.at[d, rows_at(j * 256 + first, size, 128)]
            return Gather(net, y, y_left, y_right, at(256, 0), at(128, 0), at(128, 128))
        return [gather(d) for d in (ring.early, ring.late, ring.across)]

    def x_gathers(at, order):
        return [
            Gather(net, x, x_left, x_right, at(d, 128, 0), at(d, 64, 0), at(d, 64, 64)) for d in order
        ]

    others = [(zh + d) % 4 for d in (3, 1, 2)]

    def weight_at(buf):
        return lambda d, size, first: lambda j: buf.at[d, rows_at(j * 128 + first, size, 64)]

    def weight_slot(buf):
        return lambda j, first, size: buf.at[j, rows_at(x * 128 + first, size, 64)]

    xz, uz = z_gather(xg), z_gather(ug)
    xy, uy = y_gathers(xg, xz), y_gathers(ug, uz)
    ez = Exchange(
        net, zh, z_left, z_right,
        lambda j, first, size: e_ref.at[rows_at(x * 128 + first, size, 64), rows_at(j * 512, 512, 512)],
        weight_slot(eg), relay_e, 128,
    )
    cz = Exchange(
        net, zh, z_left, z_right,
        lambda j, first, size: c_ref.at[rows_at(j * 512 + x * 128 + first, size, 64)],
        weight_slot(cg), relay_c, 128,
    )
    ex, cx = x_gathers(weight_at(eg), others), x_gathers(weight_at(cg), others)

    def hid_copy(k, slot):
        return pltpu.make_async_remote_copy(
            part.at[k, slot, 1 - c], got.at[k, slot], hid_send.at[k, slot], hid_recv.at[k, slot],
            device_id=twin, device_id_type=MESH,
        )

    def act_copy(k, slot, half):
        block = ah.at[k, half, rows_at(slot * 256, 256, 256)]
        return pltpu.make_async_remote_copy(
            block, block, act_send.at[k, slot], act_recv.at[k, slot],
            device_id=twin, device_id_type=MESH,
        )

    def partials(slot):
        where = rows_at(slot * 256, 256, 256)

        @pl.loop(0, 2)
        def _(half):
            cols = rows_at(half * 256, 256, 256)
            acc = dot(xg[0, where], eg[0, :, cols], NN)
            for j in range(1, 4):
                acc = acc + dot(xg[j, where], eg[j, :, cols], NN)
            part[0, slot, half] = acc
            acc = dot(ug[0, where], cg[0, cols], NT)
            for j in range(1, 4):
                acc = acc + dot(ug[j, where], cg[j, cols], NT)
            part[1, slot, half] = acc

        hid_copy(0, slot).start()
        hid_copy(1, slot).start()

    def pointwise(slot):
        hid_copy(0, slot).wait_recv()
        hid_copy(1, slot).wait_recv()
        bias = b_ref[row]

        @pl.loop(0, 8)
        def _(r):
            rows = rows_at(r * 32, 32, 32)
            pre = part[0, slot, c, rows] + got[0, slot, rows] + bias
            v = pre.astype(BF).astype(F32)
            back = (part[1, slot, c, rows] + got[1, slot, rows]).astype(BF).astype(F32)
            k0, k1 = 0.7978845608028654, 0.044715
            sq = v * v
            t = jnp.tanh(k0 * (v + k1 * (sq * v)))
            half = 0.5 * (1.0 + t)
            slope = half + (0.5 * v) * (1.0 - t * t) * (k0 * (1.0 + 3.0 * k1 * sq))
            out = rows_at(slot * 256 + r * 32, 32, 32)
            ah[0, c, out] = (v * half).astype(BF)
            ah[1, c, out] = (back * slope).astype(BF)

        act_copy(0, slot, c).start()
        act_copy(1, slot, c).start()

    locals_[0].wait()
    xz.start()
    locals_[1].wait()
    uz.start()
    xz.get_early()
    xy[0].start()
    ez.start()
    uz.get_early()
    uy[0].start()
    xz.get_late()
    xy[1].start()
    uz.get_late()
    uy[1].start()
    xy[0].forward()
    xz.get_across()
    ez.forward()
    ez.near()
    ex[0].start()
    ex[1].start()
    uy[0].forward()
    uz.get_across()
    xz.finish()
    xy[2].start()
    cz.start()
    ez.finish()
    ex[2].start()
    xy[1].forward()
    uz.finish()
    uy[2].start()
    ex[0].forward()
    ex[1].forward()
    uy[1].forward()
    cz.forward()
    cz.near()
    cx[0].start()
    cx[1].start()
    cz.finish()
    cx[2].start()
    ex[2].forward()
    xy[2].forward()
    cx[0].forward()
    cx[1].forward()
    cx[2].forward()
    locals_[2].wait()
    locals_[3].wait()
    for gather in ex + cx:
        gather.finish()
    partials(y)
    uy[2].forward()

    @pl.loop(0, 2)
    def _(n):
        partials((y + 1 + 2 * n) % 4)

    pointwise(y)
    for gather in xy + uy:
        gather.finish()
    partials((y + 2) % 4)

    @pl.loop(0, 3)
    def _(n):
        pointwise((y + 1 + 2 * n - n // 2 * 3) % 4)

    @pl.loop(0, 4)
    def _(slot):
        for k in range(2):
            act_copy(k, slot, 1 - c).wait_recv()
            hid_copy(k, slot).wait_send()
            act_copy(k, slot, c).wait_send()

    def reduce_to(axis, part_at, inbox, out):
        me, left, right = axis
        return Reduce(net, me, left, right, part_at, inbox, add_into,
                      lambda h, *parts: total_into(out(h), parts))

    over_x, over_y, over_z = (x, x_left, x_right), (y, y_left, y_right), (zh, z_left, z_right)
    e_red = reduce_to(over_x, lambda j, h: ge.at[j, pl.ds(2 * h, 2)], in_e, lambda h: sum_e.at[pl.ds(2 * h, 2)])
    c_red = reduce_to(over_x, lambda j, h: gc.at[j, pl.ds(2 * h, 2)], in_c, lambda h: sum_c.at[pl.ds(2 * h, 2)])

    def own_rows(s, first, size):
        return ox_ref.at[rows_at(y * 256 + s * 128 + zl * 64 + first, size, 32)]

    def per_chunk(s):
        down = reduce_to(over_y, lambda j, h: gx.at[s, j, pl.ds(2 * h, 2)], in_x.at[s],
                         lambda h: sum_x.at[s, pl.ds(2 * h, 2)])
        along = reduce_to(over_z, lambda j, h: pair_sum.at[s, j, pl.ds(32 * h, 32)], in_z.at[s],
                          lambda h: own_rows(s, 32 * h, 32))
        def at(size, first):
            return lambda j: ox_ref.at[rows_at(j * 256 + s * 128 + first, size, 64)]
        spread = Gather(net, y, y_left, y_right, at(128, 0), at(64, 0), at(64, 64))
        return down, along, spread, net.ids(2)

    chunks = [per_chunk(s) for s in range(2)]

    def out_e(j, first, size):
        return oe_ref.at[rows_at(x * 128 + first, size, 64), rows_at(j * 512, 512, 512)]

    def out_c(j, first, size):
        return oc_ref.at[rows_at(j * 512 + x * 128 + first, size, 64)]

    e_swap = Exchange(net, zh, z_left, z_right, lambda j, first, size: sum_e.at[j, pl.ds(first, size)],
                      out_e, relay_ge, 128)
    c_swap = Exchange(net, zh, z_left, z_right, lambda j, first, size: sum_c.at[j, pl.ds(first, size)],
                      out_c, relay_gc, 128)
    order = [zh] + others
    e_out = x_gathers(
        lambda d, size, first: lambda j: oe_ref.at[rows_at(j * 128 + first, size, 64), rows_at(d * 512, 512, 512)],
        order)
    c_out = x_gathers(
        lambda d, size, first: lambda j: oc_ref.at[rows_at(d * 512 + j * 128 + first, size, 64)], order)

    def pair_send(s):
        net.send(chunks[s][3][0], sum_x.at[s, :, rows_at((1 - zl) * 64, 64, 64)], pair_in.at[s], beside)

    def pair_add(s):
        net.arrived(chunks[s][3][0], pair_in.at[s], beside)

        @pl.loop(0, 4)
        def _(j):
            mine = sum_x[s, j, rows_at(zl * 64, 64, 64)].astype(F32)
            pair_sum[s, j] = (mine + pair_in[s, j].astype(F32)).astype(BF)

    def pair_back(s):
        net.send(chunks[s][3][1], own_rows(s, 0, 64), own_rows(s, 0, 64), beside)

    def pair_got(s):
        there = ox_ref.at[rows_at(y * 256 + s * 128 + (1 - zl) * 64, 64, 64)]
        net.arrived(chunks[s][3][1], there, beside)

    @pl.loop(0, 4)
    def _(j):
        for h in range(2):
            acc = (dot(xg[j], ah[1, h], TN) * factor).astype(BF)
            for q in range(4):
                ge[q, j, :, pl.ds(h * 256, 256)] = acc[q * 128:(q + 1) * 128]

    e_red.far()
    e_red.near()
    for s in range(2):
        @pl.loop(0, 4)
        def _(slot):
            where = rows_at(slot * 256 + s * 128, 128, 128)
            for j in range(4):
                acc = dot(ah[1, 0, where], eg[j, :, pl.ds(0, 256)], NT)
                acc = acc + dot(ah[1, 1, where], eg[j, :, pl.ds(256, 256)], NT)
                gx[s, slot, j] = acc.astype(BF)
        chunks[s][0].far()
        if s == 0:
            chunks[s][0].near()
    e_red.join()

    @pl.loop(0, 4)
    def _(j):
        for h in range(2):
            acc = (dot(ah[0, h], ug[j], TN) * factor).astype(BF)
            gc[2 * h, j] = acc[:128]
            gc[2 * h + 1, j] = acc[128:]

    c_red.far()
    c_red.near()
    chunks[0][0].join()
    chunks[1][0].near()

    for h in range(2):
        def add_rows(n, acc):
            block = ah[1, h, rows_at(n * 64, 64, 64)].astype(F32)
            return acc + jnp.sum(block.reshape(8, 8, 256), axis=0)
        acc = lax.fori_loop(0, 16, add_rows, jnp.zeros((8, 256), F32))
        acc = jnp.sum(acc, axis=0, keepdims=True) * factor
        small[pl.ds(0, 8), pl.ds(h * 256, 256)] = jnp.broadcast_to(acc.astype(BF).astype(F32), (8, 256))

    def add_up(n, acc):
        block = ug[zh, rows_at(n * 64, 64, 64)].astype(F32)
        return acc + jnp.sum(block.reshape(8, 8, 512), axis=0)
    acc = lax.fori_loop(0, 16, add_up, jnp.zeros((8, 512), F32))
    acc = jnp.sum(acc, axis=0, keepdims=True) * factor
    small[pl.ds(8, 8)] = jnp.broadcast_to(acc.astype(BF).astype(F32), (8, 512))
    small_k = net.ids(6)
    for n, peer in enumerate((x_right, x_left, x_across)):
        net.send(small_k[n], small, small_in.at[n], peer)

    e_red.finish()
    e_swap.start()
    oe_ref[rows_at(x * 128, 128, 128), rows_at(zh * 512, 512, 512)] = sum_e[zh]
    e_out[0].start()
    chunks[1][0].join()
    c_red.join()
    e_swap.forward()
    chunks[0][0].finish()
    pair_send(0)
    for n, peer in enumerate((x_left, x_right, x_across)):
        net.arrived(small_k[n], small_in.at[n], peer)
    whole = ((small[...] + small_in[0]) + small_in[1]) + small_in[2]
    ob_ref[zh] = whole[:8]
    oo_ref[...] = whole[8:]
    for n, peer in enumerate((z_right, z_left, z_across)):
        net.send(small_k[3 + n], ob_ref.at[zh], ob_ref.at[zh], peer)
    e_swap.near()
    e_out[1].start()
    e_out[2].start()
    pair_add(0)
    chunks[0][1].far()
    chunks[0][1].near()
    e_swap.finish()
    e_out[3].start()
    c_red.finish()
    c_swap.start()
    oc_ref[rows_at(zh * 512 + x * 128, 128, 128)] = sum_c[zh]
    c_out[0].start()
    chunks[1][0].finish()
    pair_send(1)
    chunks[0][1].join()
    e_out[0].forward()
    c_swap.forward()
    chunks[0][1].finish()
    pair_back(0)
    pair_add(1)
    chunks[1][1].far()
    chunks[1][1].near()
    e_out[1].forward()
    e_out[2].forward()
    pair_got(0)
    chunks[0][2].start()
    c_swap.near()
    c_out[1].start()
    c_out[2].start()
    chunks[1][1].join()
    e_out[3].forward()
    c_swap.finish()
    c_out[3].start()
    chunks[1][1].finish()
    pair_back(1)
    c_out[0].forward()
    chunks[0][2].forward()
    pair_got(1)
    chunks[1][2].start()
    c_out[1].forward()
    c_out[2].forward()
    chunks[1][2].forward()
    c_out[3].forward()
    for gather in e_out + c_out:
        gather.finish()
    for chunk in chunks:
        chunk[2].finish()
    for n, d in enumerate((3, 1, 2)):
        net.arrived(small_k[3 + n], ob_ref.at[(zh + d) % 4], z_across)
    net.drain()
    assert net.used <= 224


def finish(ox, oe, ob, oc, oo, gx, ge, gb, gc, go, tall, wide, sem):
    copies = [
        pltpu.make_async_copy(src, dst, sem.at[k]) for k, (src, dst) in enumerate(((oe, ge), (oc, gc), (ox, gx)))
    ]
    for copy in copies:
        copy.start()
    for k in range(4):
        cols = pl.ds(k * 128, 128)
        for j in range(4):
            tall[pl.ds(j * 4 + k, 1)] = ob[j, pl.ds(0, 1), cols]
        wide[pl.ds(k, 1)] = oo[pl.ds(0, 1), cols]
    gb[...] = tall[...].astype(BF)
    go[...] = wide[...].astype(BF)
    for copy in copies:
        copy.wait()


def local(inputs, upstream, expand, biases, contract):
    vmem = pl.BlockSpec(memory_space=pltpu.VMEM)
    anywhere = pl.BlockSpec(memory_space=pl.ANY)
    dma = pltpu.SemaphoreType.DMA
    ox, oe, ob, oc, oo = pl.pallas_call(
        kernel,
        out_shape=(
            pltpu.VMEM((1024, 512), BF),
            pltpu.VMEM((512, 2048), BF),
            pltpu.VMEM((4, 8, 512), F32),
            pltpu.VMEM((2048, 512), BF),
            pltpu.VMEM((8, 512), F32),
        ),
        in_specs=[anywhere, anywhere, anywhere, vmem, anywhere],
        out_specs=(vmem, vmem, vmem, vmem, vmem),
        scratch_shapes=[
            pltpu.VMEM((4, 1024, 512), BF),
            pltpu.VMEM((4, 1024, 512), BF),
            pltpu.VMEM((4, 512, 512), BF),
            pltpu.VMEM((4, 512, 512), BF),
            pltpu.VMEM((2, 4, 2, 256, 256), F32),
            pltpu.VMEM((2, 4, 256, 256), F32),
            pltpu.VMEM((2, 2, 1024, 256), BF),
            pltpu.VMEM((2, 64, 512), BF),
            pltpu.VMEM((2, 64, 512), BF),
            pltpu.VMEM((4, 4, 128, 512), BF),
            pltpu.VMEM((4, 4, 128, 512), BF),
            pltpu.VMEM((2, 4, 4, 128, 512), BF),
            pltpu.VMEM((6, 2, 128, 512), BF),
            pltpu.VMEM((6, 2, 128, 512), BF),
            pltpu.VMEM((2, 6, 2, 128, 512), BF),
            pltpu.VMEM((4, 128, 512), BF),
            pltpu.VMEM((4, 128, 512), BF),
            pltpu.VMEM((2, 4, 128, 512), BF),
            pltpu.VMEM((2, 64, 512), BF),
            pltpu.VMEM((2, 64, 512), BF),
            pltpu.VMEM((2, 4, 64, 512), BF),
            pltpu.VMEM((2, 4, 64, 512), BF),
            pltpu.VMEM((2, 6, 32, 512), BF),
            pltpu.VMEM((16, 512), F32),
            pltpu.VMEM((3, 16, 512), F32),
            dma((224,)),
            dma((224,)),
            dma((4,)),
            dma((2, 4)),
            dma((2, 4)),
            dma((2, 4)),
            dma((2, 4)),
        ],
        compiler_params=pltpu.CompilerParams(
            collective_id=0, has_side_effects=True, vmem_limit_bytes=50 * 1024 * 1024
        ),
    )(inputs, upstream, expand, biases.reshape(8, 1, 256), contract)
    gx, ge, gb, gc, go = pl.pallas_call(
        finish,
        out_shape=(
            jax.ShapeDtypeStruct((1024, 512), BF),
            jax.ShapeDtypeStruct((512, 2048), BF),
            jax.ShapeDtypeStruct((16, 128), BF),
            jax.ShapeDtypeStruct((2048, 512), BF),
            jax.ShapeDtypeStruct((4, 128), BF),
        ),
        in_specs=[vmem] * 5,
        out_specs=(anywhere, anywhere, vmem, anywhere, vmem),
        scratch_shapes=[pltpu.VMEM((16, 128), F32), pltpu.VMEM((4, 128), F32), dma((3,))],
        compiler_params=pltpu.CompilerParams(vmem_limit_bytes=12 * 1024 * 1024),
    )(ox, oe, ob, oc, oo)
    return gx, ge, gb.reshape(2048), gc, go.reshape(512)


def solution(mesh):
    in_specs = (P("dp", "row"), P("dp", "row"), P("row", "col"), P("col"), P("col", "row"))
    out_specs = (P("dp", "row"), P("row", "col"), P("col"), P("col", "row"), P("row"))
    return jax.shard_map(local, mesh=mesh, in_specs=in_specs, out_specs=out_specs, check_vma=False)
```

```python
import functools

import jax
import jax.numpy as jnp
from jax import lax
from jax.experimental import pallas as pl
from jax.experimental.pallas import tpu as pltpu
from jax.sharding import PartitionSpec as P

BF = jnp.bfloat16
F32 = jnp.float32
MESH = pl.DeviceIdType.MESH
NN = (((1,), (0,)), ((), ()))
NT = (((1,), (1,)), ((), ()))
TN = (((0,), (0,)), ((), ()))


def dot(a, b, dims):
    return lax.dot_general(a, b, dims, preferred_element_type=F32)


class Net:
    def __init__(self, send_sem, recv_sem):
        self.send_sem, self.recv_sem = send_sem, recv_sem
        self.used, self.sent = 0, []

    def ids(self, count):
        first = self.used
        self.used += count
        return range(first, first + count)

    def send(self, k, src, dst, device):
        copy = pltpu.make_async_remote_copy(
            src, dst, self.send_sem.at[k], self.recv_sem.at[k], device_id=device, device_id_type=MESH
        )
        copy.start()
        self.sent.append(copy)

    def arrived(self, k, dst, device):
        pltpu.make_async_remote_copy(
            dst, dst, self.send_sem.at[k], self.recv_sem.at[k], device_id=device, device_id_type=MESH
        ).wait_recv()

    def drain(self):
        for copy in self.sent:
            copy.wait_send()


class Gather:
    def __init__(self, net, me, left, right, full, top, bottom):
        self.net, self.me, self.left, self.right = net, me, left, right
        self.full, self.top, self.bottom = full, top, bottom
        self.k = net.ids(4)

    def start(self):
        block = self.full(self.me)
        self.net.send(self.k[0], block, block, self.right)
        self.net.send(self.k[1], block, block, self.left)

    def near(self):
        self.net.arrived(self.k[0], self.full((self.me + 3) % 4), self.left)
        self.net.arrived(self.k[1], self.full((self.me + 1) % 4), self.right)

    def forward(self):
        before, after = (self.me + 3) % 4, (self.me + 1) % 4
        self.net.arrived(self.k[0], self.full(before), self.left)
        self.net.send(self.k[2], self.top(before), self.top(before), self.right)
        self.net.arrived(self.k[1], self.full(after), self.right)
        self.net.send(self.k[3], self.bottom(after), self.bottom(after), self.left)

    def finish(self):
        across = (self.me + 2) % 4
        self.net.arrived(self.k[2], self.top(across), self.left)
        self.net.arrived(self.k[3], self.bottom(across), self.right)


class Exchange:
    def __init__(self, net, me, left, right, src, dst, relay, rows):
        self.net, self.me, self.left, self.right = net, me, left, right
        self.src, self.dst, self.relay, self.rows = src, dst, relay, rows
        self.k = net.ids(6)

    def start(self):
        me, half = self.me, self.rows // 2
        before, after, across = (me + 3) % 4, (me + 1) % 4, (me + 2) % 4
        self.net.send(self.k[2], self.src(across, 0, half), self.relay.at[0], self.right)
        self.net.send(self.k[3], self.src(across, half, half), self.relay.at[1], self.left)
        self.net.send(self.k[0], self.src(after, 0, self.rows), self.dst(me, 0, self.rows), self.right)
        self.net.send(self.k[1], self.src(before, 0, self.rows), self.dst(me, 0, self.rows), self.left)

    def forward(self):
        me, half = self.me, self.rows // 2
        before, after = (me + 3) % 4, (me + 1) % 4
        self.net.arrived(self.k[2], self.relay.at[0], self.left)
        self.net.send(self.k[4], self.relay.at[0], self.dst(before, 0, half), self.right)
        self.net.arrived(self.k[3], self.relay.at[1], self.right)
        self.net.send(self.k[5], self.relay.at[1], self.dst(after, half, half), self.left)

    def near(self):
        me = self.me
        self.net.arrived(self.k[0], self.dst((me + 3) % 4, 0, self.rows), self.left)
        self.net.arrived(self.k[1], self.dst((me + 1) % 4, 0, self.rows), self.right)

    def finish(self):
        half, across = self.rows // 2, (self.me + 2) % 4
        self.net.arrived(self.k[4], self.dst(across, 0, half), self.left)
        self.net.arrived(self.k[5], self.dst(across, half, half), self.right)


class Reduce:
    def __init__(self, net, me, left, right, part, inbox, add, total):
        self.net, self.me, self.left, self.right = net, me, left, right
        self.part, self.inbox, self.add, self.total = part, inbox, add, total
        self.k = net.ids(6)

    def far(self):
        across = (self.me + 2) % 4
        self.net.send(self.k[0], self.part(across, 0), self.inbox.at[0], self.right)
        self.net.send(self.k[1], self.part(across, 1), self.inbox.at[1], self.left)

    def near(self):
        before, after = (self.me + 3) % 4, (self.me + 1) % 4
        self.net.send(self.k[2], self.part(after, 1), self.inbox.at[2], self.right)
        self.net.send(self.k[3], self.part(before, 0), self.inbox.at[3], self.left)

    def join(self):
        before, after = (self.me + 3) % 4, (self.me + 1) % 4
        self.net.arrived(self.k[0], self.inbox.at[0], self.left)
        self.add(self.part(after, 0), self.inbox.at[0])
        self.net.send(self.k[4], self.part(after, 0), self.inbox.at[4], self.right)
        self.net.arrived(self.k[1], self.inbox.at[1], self.right)
        self.add(self.part(before, 1), self.inbox.at[1])
        self.net.send(self.k[5], self.part(before, 1), self.inbox.at[5], self.left)

    def finish(self):
        self.net.arrived(self.k[3], self.inbox.at[3], self.right)
        self.net.arrived(self.k[4], self.inbox.at[4], self.left)
        self.total(0, self.part(self.me, 0), self.inbox.at[3], self.inbox.at[4])
        self.net.arrived(self.k[2], self.inbox.at[2], self.left)
        self.net.arrived(self.k[5], self.inbox.at[5], self.right)
        self.total(1, self.part(self.me, 1), self.inbox.at[2], self.inbox.at[5])


def add_into(target, other):
    rows = min(64, target.shape[-2])
    lead = target.shape[0] if len(target.shape) == 3 else 1
    depth = target.shape[-2]

    def view(ref, i, r):
        where = pl.ds(pl.multiple_of(r * rows, rows), rows)
        return ref.at[i, where] if len(ref.shape) == 3 else ref.at[where]

    @pl.loop(0, lead * (depth // rows))
    def _(n):
        i, r = n // (depth // rows), n % (depth // rows)
        mine = view(target, i, r)
        mine[...] = (mine[...].astype(F32) + view(other, i, r)[...].astype(F32)).astype(BF)


def total_into(out, parts):
    rows = min(64, out.shape[-2])
    lead = out.shape[0] if len(out.shape) == 3 else 1
    depth = out.shape[-2]

    def view(ref, i, r):
        where = pl.ds(pl.multiple_of(r * rows, rows), rows)
        return ref.at[i, where] if len(ref.shape) == 3 else ref.at[where]

    @pl.loop(0, lead * (depth // rows))
    def _(n):
        i, r = n // (depth // rows), n % (depth // rows)
        acc = view(parts[0], i, r)[...].astype(F32)
        for other in parts[1:]:
            acc = acc + view(other, i, r)[...].astype(F32)
        view(out, i, r)[...] = acc.astype(BF)


def rows_at(start, size, unit):
    return pl.ds(pl.multiple_of(start, unit), size)


class PairRing:
    def __init__(self, net, zh, zl, outer, inner, block):
        self.net, self.outer, self.inner, self.block = net, outer, inner, block
        self.own, self.across = zh, (zh + 2) % 4
        self.early, self.late = (zh + 3 + 2 * zl) % 4, (zh + 5 - 2 * zl) % 4
        self.out_half, self.in_half = (1 - zl) * 128, zl * 128
        self.k = net.ids(4)

    def send(self, k, block, device):
        self.net.send(self.k[k], block, block, device)

    def start(self):
        self.send(0, self.block(self.own, 0, 256), self.outer)

    def get_early(self):
        block = self.block(self.early, 0, 256)
        self.net.arrived(self.k[0], block, self.outer)
        self.send(1, block, self.inner)

    def get_late(self):
        self.net.arrived(self.k[1], self.block(self.late, 0, 256), self.inner)
        self.send(2, self.block(self.late, self.out_half, 128), self.outer)

    def get_across(self):
        block = self.block(self.across, self.in_half, 128)
        self.net.arrived(self.k[2], block, self.outer)
        self.send(3, block, self.inner)

    def finish(self):
        self.net.arrived(self.k[3], self.block(self.across, self.out_half, 128), self.inner)


def kernel(
    x_ref, u_ref, e_ref, b_ref, c_ref,
    ox_ref, oe_ref, ob_ref, oc_ref, oo_ref,
    xg, ug, eg, cg, part, got, ah, relay_e, relay_c,
    ge, gc, gx, in_e, in_c, in_x, sum_e, sum_c, sum_x, relay_ge, relay_gc,
    pair_in, pair_sum, in_z, small, small_in,
    send_sem, recv_sem, local_sem, hid_send, hid_recv, act_send, act_recv,
):
    row, col, x = lax.axis_index("row"), lax.axis_index("col"), lax.axis_index("dp")
    zh, c = row // 2, row % 2
    y, zl = col // 2, col % 2
    factor = 1.0 / 64.0

    z_right, z_left = {"row": ((zh + 1) % 4) * 2 + c}, {"row": ((zh + 3) % 4) * 2 + c}
    z_across = {"row": ((zh + 2) % 4) * 2 + c}
    y_right, y_left = {"col": ((y + 1) % 4) * 2 + zl}, {"col": ((y + 3) % 4) * 2 + zl}
    x_right, x_left, x_across = {"dp": (x + 1) % 4}, {"dp": (x + 3) % 4}, {"dp": (x + 2) % 4}
    twin = {"row": zh * 2 + 1 - c}
    beside = {"col": y * 2 + 1 - zl}
    outer = {"row": ((zh + 3 + 2 * zl) % 4) * 2 + c, "col": y * 2 + 1 - zl}

    locals_ = [
        pltpu.make_async_copy(x_ref, xg.at[zh], local_sem.at[0]),
        pltpu.make_async_copy(u_ref, ug.at[zh], local_sem.at[1]),
        pltpu.make_async_copy(e_ref.at[:, rows_at(zh * 512, 512, 512)], eg.at[zh], local_sem.at[2]),
        pltpu.make_async_copy(c_ref.at[rows_at(zh * 512, 512, 512)], cg.at[zh], local_sem.at[3]),
    ]
    for copy in locals_:
        copy.start()

    barrier = pltpu.get_barrier_semaphore()
    peers = (z_right, z_left, z_across, y_right, y_left, x_right, x_left, x_across, twin, beside, outer)
    for peer in peers:
        pl.semaphore_signal(barrier, inc=1, device_id=peer, device_id_type=MESH)
    pl.semaphore_wait(barrier, len(peers))

    net = Net(send_sem, recv_sem)

    def z_gather(buf, slot):
        return PairRing(
            net, zh, zl, outer, beside, lambda j, first, size: buf.at[j, rows_at(slot * 256 + first, size, 128)]
        )

    def y_gathers(buf, ring):
        def gather(d):
            def at(size, first):
                return lambda j: buf.at[d, rows_at(j * 256 + first, size, 128)]
            return Gather(net, y, y_left, y_right, at(256, 0), at(128, 0), at(128, 128))
        return [gather(d) for d in (ring.early, ring.late, ring.across)]

    def x_gathers(at, order):
        return [
            Gather(net, x, x_left, x_right, at(d, 128, 0), at(d, 64, 0), at(d, 64, 64)) for d in order
        ]

    others = [(zh + d) % 4 for d in (3, 1, 2)]

    def weight_at(buf):
        return lambda d, size, first: lambda j: buf.at[d, rows_at(j * 128 + first, size, 64)]

    def weight_slot(buf):
        return lambda j, first, size: buf.at[j, rows_at(x * 128 + first, size, 64)]

    xz, uz = z_gather(xg, y), z_gather(ug, y)
    xy, uy = y_gathers(xg, xz), y_gathers(ug, uz)
    ez = Exchange(
        net, zh, z_left, z_right,
        lambda j, first, size: e_ref.at[rows_at(x * 128 + first, size, 64), rows_at(j * 512, 512, 512)],
        weight_slot(eg), relay_e, 128,
    )
    cz = Exchange(
        net, zh, z_left, z_right,
        lambda j, first, size: c_ref.at[rows_at(j * 512 + x * 128 + first, size, 64)],
        weight_slot(cg), relay_c, 128,
    )
    ex, cx = x_gathers(weight_at(eg), others), x_gathers(weight_at(cg), others)

    def hid_copy(k, slot):
        return pltpu.make_async_remote_copy(
            part.at[k, slot, 1 - c], got.at[k, slot], hid_send.at[k, slot], hid_recv.at[k, slot],
            device_id=twin, device_id_type=MESH,
        )

    def act_copy(k, slot, half):
        block = ah.at[k, half, rows_at(slot * 256, 256, 256)]
        return pltpu.make_async_remote_copy(
            block, block, act_send.at[k, slot], act_recv.at[k, slot],
            device_id=twin, device_id_type=MESH,
        )

    def partials(slot):
        where = rows_at(slot * 256, 256, 256)

        @pl.loop(0, 2)
        def _(half):
            cols = rows_at(half * 256, 256, 256)
            acc = dot(xg[0, where], eg[0, :, cols], NN)
            for j in range(1, 4):
                acc = acc + dot(xg[j, where], eg[j, :, cols], NN)
            part[0, slot, half] = acc
            acc = dot(ug[0, where], cg[0, cols], NT)
            for j in range(1, 4):
                acc = acc + dot(ug[j, where], cg[j, cols], NT)
            part[1, slot, half] = acc

        hid_copy(0, slot).start()
        hid_copy(1, slot).start()

    def pointwise(slot):
        hid_copy(0, slot).wait_recv()
        hid_copy(1, slot).wait_recv()
        bias = b_ref[row]

        @pl.loop(0, 8)
        def _(r):
            rows = rows_at(r * 32, 32, 32)
            pre = part[0, slot, c, rows] + got[0, slot, rows] + bias
            v = pre.astype(BF).astype(F32)
            back = (part[1, slot, c, rows] + got[1, slot, rows]).astype(BF).astype(F32)
            k0, k1 = 0.7978845608028654, 0.044715
            sq = v * v
            t = jnp.tanh(k0 * (v + k1 * (sq * v)))
            half = 0.5 * (1.0 + t)
            slope = half + (0.5 * v) * (1.0 - t * t) * (k0 * (1.0 + 3.0 * k1 * sq))
            out = rows_at(slot * 256 + r * 32, 32, 32)
            ah[0, c, out] = (v * half).astype(BF)
            ah[1, c, out] = (back * slope).astype(BF)

        act_copy(0, slot, c).start()
        act_copy(1, slot, c).start()

    def hidden_done():
        @pl.loop(0, 4)
        def _(slot):
            for k in range(2):
                act_copy(k, slot, 1 - c).wait_recv()
                hid_copy(k, slot).wait_send()
                act_copy(k, slot, c).wait_send()

    def reduce_to(axis, part_at, inbox, out):
        me, left, right = axis
        return Reduce(net, me, left, right, part_at, inbox, add_into,
                      lambda h, *parts: total_into(out(h), parts))

    over_x, over_y, over_z = (x, x_left, x_right), (y, y_left, y_right), (zh, z_left, z_right)
    e_red = reduce_to(over_x, lambda j, h: ge.at[j, pl.ds(2 * h, 2)], in_e, lambda h: sum_e.at[pl.ds(2 * h, 2)])
    c_red = reduce_to(over_x, lambda j, h: gc.at[j, pl.ds(2 * h, 2)], in_c, lambda h: sum_c.at[pl.ds(2 * h, 2)])

    def own_rows(s, first, size):
        return ox_ref.at[rows_at(y * 256 + s * 128 + zl * 64 + first, size, 32)]

    def per_chunk(s):
        down = reduce_to(over_y, lambda j, h: gx.at[s, j, pl.ds(2 * h, 2)], in_x.at[s],
                         lambda h: sum_x.at[s, pl.ds(2 * h, 2)])
        along = reduce_to(over_z, lambda j, h: pair_sum.at[s, j, pl.ds(32 * h, 32)], in_z.at[s],
                          lambda h: own_rows(s, 32 * h, 32))
        def at(size, first):
            return lambda j: ox_ref.at[rows_at(j * 256 + s * 128 + first, size, 64)]
        spread = Gather(net, y, y_left, y_right, at(128, 0), at(64, 0), at(64, 64))
        return down, along, spread, net.ids(2)

    chunks = [per_chunk(s) for s in range(2)]

    def out_e(j, first, size):
        return oe_ref.at[rows_at(x * 128 + first, size, 64), rows_at(j * 512, 512, 512)]

    def out_c(j, first, size):
        return oc_ref.at[rows_at(j * 512 + x * 128 + first, size, 64)]

    e_swap = Exchange(net, zh, z_left, z_right, lambda j, first, size: sum_e.at[j, pl.ds(first, size)],
                      out_e, relay_ge, 128)
    c_swap = Exchange(net, zh, z_left, z_right, lambda j, first, size: sum_c.at[j, pl.ds(first, size)],
                      out_c, relay_gc, 128)
    order = [zh] + others
    e_out = x_gathers(
        lambda d, size, first: lambda j: oe_ref.at[rows_at(j * 128 + first, size, 64), rows_at(d * 512, 512, 512)],
        order)
    c_out = x_gathers(
        lambda d, size, first: lambda j: oc_ref.at[rows_at(d * 512 + j * 128 + first, size, 64)], order)

    def pair_send(s):
        net.send(chunks[s][3][0], sum_x.at[s, :, rows_at((1 - zl) * 64, 64, 64)], pair_in.at[s], beside)

    def pair_add(s):
        net.arrived(chunks[s][3][0], pair_in.at[s], beside)

        @pl.loop(0, 4)
        def _(j):
            mine = sum_x[s, j, rows_at(zl * 64, 64, 64)].astype(F32)
            pair_sum[s, j] = (mine + pair_in[s, j].astype(F32)).astype(BF)

    def pair_back(s):
        net.send(chunks[s][3][1], own_rows(s, 0, 64), own_rows(s, 0, 64), beside)

    def pair_got(s):
        there = ox_ref.at[rows_at(y * 256 + s * 128 + (1 - zl) * 64, 64, 64)]
        net.arrived(chunks[s][3][1], there, beside)

    small_k = net.ids(6)

    def grad_expand():
        @pl.loop(0, 4)
        def _(j):
            for h in range(2):
                acc = (dot(xg[j], ah[1, h], TN) * factor).astype(BF)
                for q in range(4):
                    ge[q, j, :, pl.ds(h * 256, 256)] = acc[q * 128:(q + 1) * 128]

    def grad_contract():
        @pl.loop(0, 4)
        def _(j):
            for h in range(2):
                acc = (dot(ah[0, h], ug[j], TN) * factor).astype(BF)
                gc[2 * h, j] = acc[:128]
                gc[2 * h + 1, j] = acc[128:]

    def grad_tokens(s):
        @pl.loop(0, 4)
        def _(j):
            first = ah[1, 0].reshape(4, 2, 128, 256)[:, s].reshape(512, 256)
            second = ah[1, 1].reshape(4, 2, 128, 256)[:, s].reshape(512, 256)
            acc = dot(first, eg[j, :, pl.ds(0, 256)], NT) + dot(second, eg[j, :, pl.ds(256, 256)], NT)
            acc = acc.astype(BF)
            for slot in range(4):
                gx[s, slot, j] = acc[slot * 128:(slot + 1) * 128]

    def token_sums():
        for h in range(2):
            def add_rows(n, acc):
                block = ah[1, h, rows_at(n * 64, 64, 64)].astype(F32)
                return acc + jnp.sum(block.reshape(8, 8, 256), axis=0)
            acc = lax.fori_loop(0, 16, add_rows, jnp.zeros((8, 256), F32))
            acc = jnp.sum(acc, axis=0, keepdims=True) * factor
            small[pl.ds(0, 8), pl.ds(h * 256, 256)] = jnp.broadcast_to(acc.astype(BF).astype(F32), (8, 256))

        def add_up(n, acc):
            block = ug[zh, rows_at(n * 64, 64, 64)].astype(F32)
            return acc + jnp.sum(block.reshape(8, 8, 512), axis=0)
        acc = lax.fori_loop(0, 16, add_up, jnp.zeros((8, 512), F32))
        acc = jnp.sum(acc, axis=0, keepdims=True) * factor
        small[pl.ds(8, 8)] = jnp.broadcast_to(acc.astype(BF).astype(F32), (8, 512))
        for n, peer in enumerate((x_right, x_left, x_across)):
            net.send(small_k[n], small, small_in.at[n], peer)

    def small_sums():
        for n, peer in enumerate((x_left, x_right, x_across)):
            net.arrived(small_k[n], small_in.at[n], peer)
        whole = ((small[...] + small_in[0]) + small_in[1]) + small_in[2]
        ob_ref[zh] = whole[:8]
        oo_ref[...] = whole[8:]
        for n, peer in enumerate((z_right, z_left, z_across)):
            net.send(small_k[3 + n], ob_ref.at[zh], ob_ref.at[zh], peer)

    locals_[0].wait()
    xz.start()
    locals_[1].wait()
    uz.start()
    xz.get_early()
    xy[0].start()
    ez.start()
    uz.get_early()
    uy[0].start()
    xy[0].forward()
    uy[0].forward()
    ez.near()
    ex[0].start()
    ex[1].start()
    xz.get_late()
    xy[1].start()
    ez.forward()
    cz.start()
    uz.get_late()
    uy[1].start()
    xy[1].forward()
    ez.finish()
    ex[2].start()
    ex[2].forward()
    xz.get_across()
    cz.forward()
    ex[0].forward()
    ex[1].forward()
    uy[1].forward()
    cz.near()
    cx[0].start()
    cx[1].start()
    xz.finish()
    xy[2].start()
    uz.get_across()
    cz.finish()
    cx[2].start()
    uz.finish()
    uy[2].start()
    cx[0].forward()
    cx[1].forward()
    cx[2].forward()
    xy[2].forward()
    uy[2].forward()
    locals_[2].wait()
    locals_[3].wait()
    for gather in ex + cx:
        gather.finish()
    partials((y + 1) % 4)
    partials((y + 3) % 4)
    partials(y)
    for gather in xy + uy:
        gather.finish()
    partials((y + 2) % 4)
    pointwise((y + 1) % 4)
    pointwise((y + 3) % 4)
    pointwise(y)
    pointwise((y + 2) % 4)
    hidden_done()
    grad_tokens(0)
    chunks[0][0].far()
    grad_expand()
    e_red.far()
    chunks[0][0].near()
    grad_tokens(1)
    chunks[0][0].join()
    chunks[1][0].far()
    e_red.near()
    chunks[1][0].near()
    grad_contract()
    e_red.join()
    c_red.far()
    chunks[0][0].finish()
    pair_send(0)
    e_red.finish()
    oe_ref[rows_at(x * 128, 128, 128), rows_at(zh * 512, 512, 512)] = sum_e[zh]
    e_swap.start()
    c_red.near()
    chunks[1][0].join()
    pair_add(0)
    chunks[0][1].far()
    chunks[0][1].near()
    c_red.join()
    e_out[0].start()
    chunks[1][0].finish()
    pair_send(1)
    c_red.finish()
    oc_ref[rows_at(zh * 512 + x * 128, 128, 128)] = sum_c[zh]
    c_out[0].start()
    e_out[0].forward()
    c_swap.start()
    token_sums()
    pair_add(1)
    chunks[1][1].far()
    chunks[1][1].near()
    chunks[0][1].join()
    e_swap.near()
    e_out[1].start()
    e_out[2].start()
    c_out[0].forward()
    e_out[2].forward()
    e_swap.forward()
    c_swap.near()
    c_out[1].start()
    c_out[2].start()
    chunks[1][1].join()
    e_out[1].forward()
    chunks[0][1].finish()
    pair_back(0)
    c_swap.forward()
    e_swap.finish()
    e_out[3].start()
    chunks[1][1].finish()
    pair_back(1)
    pair_got(0)
    chunks[0][2].start()
    c_out[2].forward()
    c_swap.finish()
    c_out[3].start()
    small_sums()
    c_out[1].forward()
    pair_got(1)
    chunks[1][2].start()
    chunks[0][2].forward()
    e_out[3].forward()
    c_out[3].forward()
    chunks[1][2].forward()
    for gather in e_out + c_out:
        gather.finish()
    for chunk in chunks:
        chunk[2].finish()
    for n, d in enumerate((3, 1, 2)):
        net.arrived(small_k[3 + n], ob_ref.at[(zh + d) % 4], z_across)
    net.drain()
    assert net.used <= 224


def finish(ox, oe, ob, oc, oo, gx, ge, gb, gc, go, tall, wide, sem):
    copies = [
        pltpu.make_async_copy(src, dst, sem.at[k]) for k, (src, dst) in enumerate(((oe, ge), (oc, gc), (ox, gx)))
    ]
    for copy in copies:
        copy.start()
    for k in range(4):
        cols = pl.ds(k * 128, 128)
        for j in range(4):
            tall[pl.ds(j * 4 + k, 1)] = ob[j, pl.ds(0, 1), cols]
        wide[pl.ds(k, 1)] = oo[pl.ds(0, 1), cols]
    gb[...] = tall[...].astype(BF)
    go[...] = wide[...].astype(BF)
    for copy in copies:
        copy.wait()


def local(inputs, upstream, expand, biases, contract):
    vmem = pl.BlockSpec(memory_space=pltpu.VMEM)
    anywhere = pl.BlockSpec(memory_space=pl.ANY)
    dma = pltpu.SemaphoreType.DMA
    ox, oe, ob, oc, oo = pl.pallas_call(
        kernel,
        out_shape=(
            pltpu.VMEM((1024, 512), BF),
            pltpu.VMEM((512, 2048), BF),
            pltpu.VMEM((4, 8, 512), F32),
            pltpu.VMEM((2048, 512), BF),
            pltpu.VMEM((8, 512), F32),
        ),
        in_specs=[anywhere, anywhere, anywhere, vmem, anywhere],
        out_specs=(vmem, vmem, vmem, vmem, vmem),
        scratch_shapes=[
            pltpu.VMEM((4, 1024, 512), BF),
            pltpu.VMEM((4, 1024, 512), BF),
            pltpu.VMEM((4, 512, 512), BF),
            pltpu.VMEM((4, 512, 512), BF),
            pltpu.VMEM((2, 4, 2, 256, 256), F32),
            pltpu.VMEM((2, 4, 256, 256), F32),
            pltpu.VMEM((2, 2, 1024, 256), BF),
            pltpu.VMEM((2, 64, 512), BF),
            pltpu.VMEM((2, 64, 512), BF),
            pltpu.VMEM((4, 4, 128, 512), BF),
            pltpu.VMEM((4, 4, 128, 512), BF),
            pltpu.VMEM((2, 4, 4, 128, 512), BF),
            pltpu.VMEM((6, 2, 128, 512), BF),
            pltpu.VMEM((6, 2, 128, 512), BF),
            pltpu.VMEM((2, 6, 2, 128, 512), BF),
            pltpu.VMEM((4, 128, 512), BF),
            pltpu.VMEM((4, 128, 512), BF),
            pltpu.VMEM((2, 4, 128, 512), BF),
            pltpu.VMEM((2, 64, 512), BF),
            pltpu.VMEM((2, 64, 512), BF),
            pltpu.VMEM((2, 4, 64, 512), BF),
            pltpu.VMEM((2, 4, 64, 512), BF),
            pltpu.VMEM((2, 6, 32, 512), BF),
            pltpu.VMEM((16, 512), F32),
            pltpu.VMEM((3, 16, 512), F32),
            dma((224,)),
            dma((224,)),
            dma((4,)),
            dma((2, 4)),
            dma((2, 4)),
            dma((2, 4)),
            dma((2, 4)),
        ],
        compiler_params=pltpu.CompilerParams(
            collective_id=0, has_side_effects=True, vmem_limit_bytes=50 * 1024 * 1024
        ),
    )(inputs, upstream, expand, biases.reshape(8, 1, 256), contract)
    gx, ge, gb, gc, go = pl.pallas_call(
        finish,
        out_shape=(
            jax.ShapeDtypeStruct((1024, 512), BF),
            jax.ShapeDtypeStruct((512, 2048), BF),
            jax.ShapeDtypeStruct((16, 128), BF),
            jax.ShapeDtypeStruct((2048, 512), BF),
            jax.ShapeDtypeStruct((4, 128), BF),
        ),
        in_specs=[vmem] * 5,
        out_specs=(anywhere, anywhere, vmem, anywhere, vmem),
        scratch_shapes=[pltpu.VMEM((16, 128), F32), pltpu.VMEM((4, 128), F32), dma((3,))],
        compiler_params=pltpu.CompilerParams(vmem_limit_bytes=12 * 1024 * 1024),
    )(ox, oe, ob, oc, oo)
    return gx, ge, gb.reshape(2048), gc, go.reshape(512)


def solution(mesh):
    in_specs = (P("dp", "row"), P("dp", "row"), P("row", "col"), P("col"), P("col", "row"))
    out_specs = (P("dp", "row"), P("row", "col"), P("col"), P("col", "row"), P("row"))
    return jax.shard_map(local, mesh=mesh, in_specs=in_specs, out_specs=out_specs, check_vma=False)
```

```python
import functools

import jax
import jax.numpy as jnp
from jax import lax
from jax.experimental import pallas as pl
from jax.experimental.pallas import tpu as pltpu
from jax.sharding import PartitionSpec as P

BF = jnp.bfloat16
F32 = jnp.float32
MESH = pl.DeviceIdType.MESH
NN = (((1,), (0,)), ((), ()))
NT = (((1,), (1,)), ((), ()))
TN = (((0,), (0,)), ((), ()))


def dot(a, b, dims):
    return lax.dot_general(a, b, dims, preferred_element_type=F32)


class Net:
    def __init__(self, send_sem, recv_sem):
        self.send_sem, self.recv_sem = send_sem, recv_sem
        self.used, self.sent = 0, []

    def ids(self, count):
        first = self.used
        self.used += count
        return range(first, first + count)

    def send(self, k, src, dst, device):
        copy = pltpu.make_async_remote_copy(
            src, dst, self.send_sem.at[k], self.recv_sem.at[k], device_id=device, device_id_type=MESH
        )
        copy.start()
        self.sent.append(copy)

    def arrived(self, k, dst, device):
        pltpu.make_async_remote_copy(
            dst, dst, self.send_sem.at[k], self.recv_sem.at[k], device_id=device, device_id_type=MESH
        ).wait_recv()

    def drain(self):
        for copy in self.sent:
            copy.wait_send()


class Gather:
    def __init__(self, net, me, left, right, full, top, bottom):
        self.net, self.me, self.left, self.right = net, me, left, right
        self.full, self.top, self.bottom = full, top, bottom
        self.k = net.ids(4)

    def start(self):
        block = self.full(self.me)
        self.net.send(self.k[0], block, block, self.right)
        self.net.send(self.k[1], block, block, self.left)

    def near(self):
        self.net.arrived(self.k[0], self.full((self.me + 3) % 4), self.left)
        self.net.arrived(self.k[1], self.full((self.me + 1) % 4), self.right)

    def forward(self):
        before, after = (self.me + 3) % 4, (self.me + 1) % 4
        self.net.arrived(self.k[0], self.full(before), self.left)
        self.net.send(self.k[2], self.top(before), self.top(before), self.right)
        self.net.arrived(self.k[1], self.full(after), self.right)
        self.net.send(self.k[3], self.bottom(after), self.bottom(after), self.left)

    def finish(self):
        across = (self.me + 2) % 4
        self.net.arrived(self.k[2], self.top(across), self.left)
        self.net.arrived(self.k[3], self.bottom(across), self.right)


class Exchange:
    def __init__(self, net, me, left, right, src, dst, relay, rows):
        self.net, self.me, self.left, self.right = net, me, left, right
        self.src, self.dst, self.relay, self.rows = src, dst, relay, rows
        self.k = net.ids(6)

    def start(self):
        me, half = self.me, self.rows // 2
        before, after, across = (me + 3) % 4, (me + 1) % 4, (me + 2) % 4
        self.net.send(self.k[2], self.src(across, 0, half), self.relay.at[0], self.right)
        self.net.send(self.k[3], self.src(across, half, half), self.relay.at[1], self.left)
        self.net.send(self.k[0], self.src(after, 0, self.rows), self.dst(me, 0, self.rows), self.right)
        self.net.send(self.k[1], self.src(before, 0, self.rows), self.dst(me, 0, self.rows), self.left)

    def forward(self):
        me, half = self.me, self.rows // 2
        before, after = (me + 3) % 4, (me + 1) % 4
        self.net.arrived(self.k[2], self.relay.at[0], self.left)
        self.net.send(self.k[4], self.relay.at[0], self.dst(before, 0, half), self.right)
        self.net.arrived(self.k[3], self.relay.at[1], self.right)
        self.net.send(self.k[5], self.relay.at[1], self.dst(after, half, half), self.left)

    def near(self):
        me = self.me
        self.net.arrived(self.k[0], self.dst((me + 3) % 4, 0, self.rows), self.left)
        self.net.arrived(self.k[1], self.dst((me + 1) % 4, 0, self.rows), self.right)

    def finish(self):
        half, across = self.rows // 2, (self.me + 2) % 4
        self.net.arrived(self.k[4], self.dst(across, 0, half), self.left)
        self.net.arrived(self.k[5], self.dst(across, half, half), self.right)


class Reduce:
    def __init__(self, net, me, left, right, part, inbox, add, total):
        self.net, self.me, self.left, self.right = net, me, left, right
        self.part, self.inbox, self.add, self.total = part, inbox, add, total
        self.k = net.ids(6)

    def far(self):
        across = (self.me + 2) % 4
        self.net.send(self.k[0], self.part(across, 0), self.inbox.at[0], self.right)
        self.net.send(self.k[1], self.part(across, 1), self.inbox.at[1], self.left)

    def near(self):
        before, after = (self.me + 3) % 4, (self.me + 1) % 4
        self.net.send(self.k[2], self.part(after, 1), self.inbox.at[2], self.right)
        self.net.send(self.k[3], self.part(before, 0), self.inbox.at[3], self.left)

    def join(self):
        before, after = (self.me + 3) % 4, (self.me + 1) % 4
        self.net.arrived(self.k[0], self.inbox.at[0], self.left)
        self.add(self.part(after, 0), self.inbox.at[0])
        self.net.send(self.k[4], self.part(after, 0), self.inbox.at[4], self.right)
        self.net.arrived(self.k[1], self.inbox.at[1], self.right)
        self.add(self.part(before, 1), self.inbox.at[1])
        self.net.send(self.k[5], self.part(before, 1), self.inbox.at[5], self.left)

    def finish(self):
        self.net.arrived(self.k[3], self.inbox.at[3], self.right)
        self.net.arrived(self.k[4], self.inbox.at[4], self.left)
        self.total(0, self.part(self.me, 0), self.inbox.at[3], self.inbox.at[4])
        self.net.arrived(self.k[2], self.inbox.at[2], self.left)
        self.net.arrived(self.k[5], self.inbox.at[5], self.right)
        self.total(1, self.part(self.me, 1), self.inbox.at[2], self.inbox.at[5])


def add_into(target, other):
    rows = min(64, target.shape[-2])
    lead = target.shape[0] if len(target.shape) == 3 else 1
    depth = target.shape[-2]

    def view(ref, i, r):
        where = pl.ds(pl.multiple_of(r * rows, rows), rows)
        return ref.at[i, where] if len(ref.shape) == 3 else ref.at[where]

    @pl.loop(0, lead * (depth // rows))
    def _(n):
        i, r = n // (depth // rows), n % (depth // rows)
        mine = view(target, i, r)
        mine[...] = (mine[...].astype(F32) + view(other, i, r)[...].astype(F32)).astype(BF)


def total_into(out, parts):
    rows = min(64, out.shape[-2])
    lead = out.shape[0] if len(out.shape) == 3 else 1
    depth = out.shape[-2]

    def view(ref, i, r):
        where = pl.ds(pl.multiple_of(r * rows, rows), rows)
        return ref.at[i, where] if len(ref.shape) == 3 else ref.at[where]

    @pl.loop(0, lead * (depth // rows))
    def _(n):
        i, r = n // (depth // rows), n % (depth // rows)
        acc = view(parts[0], i, r)[...].astype(F32)
        for other in parts[1:]:
            acc = acc + view(other, i, r)[...].astype(F32)
        view(out, i, r)[...] = acc.astype(BF)


def rows_at(start, size, unit):
    return pl.ds(pl.multiple_of(start, unit), size)


class PairRing:
    def __init__(self, net, zh, zl, outer, inner, block):
        self.net, self.outer, self.inner, self.block = net, outer, inner, block
        self.own, self.across = zh, (zh + 2) % 4
        self.early, self.late = (zh + 3 + 2 * zl) % 4, (zh + 5 - 2 * zl) % 4
        self.out_half, self.in_half = (1 - zl) * 128, zl * 128
        self.k = net.ids(4)

    def send(self, k, block, device):
        self.net.send(self.k[k], block, block, device)

    def start(self):
        self.send(0, self.block(self.own, 0, 256), self.outer)

    def get_early(self):
        block = self.block(self.early, 0, 256)
        self.net.arrived(self.k[0], block, self.outer)
        self.send(1, block, self.inner)

    def get_late(self):
        self.net.arrived(self.k[1], self.block(self.late, 0, 256), self.inner)
        self.send(2, self.block(self.late, self.out_half, 128), self.outer)

    def get_across(self):
        block = self.block(self.across, self.in_half, 128)
        self.net.arrived(self.k[2], block, self.outer)
        self.send(3, block, self.inner)

    def finish(self):
        self.net.arrived(self.k[3], self.block(self.across, self.out_half, 128), self.inner)


def kernel(
    x_ref, u_ref, e_ref, b_ref, c_ref,
    ox_ref, oe_ref, ob_ref, oc_ref, oo_ref,
    xg, ug, eg, cg, part, got, ah, relay_e, relay_c,
    ge, gc, gx, in_e, in_c, in_x, sum_e, sum_c, sum_x, relay_ge, relay_gc,
    pair_in, pair_sum, in_z, small, small_in, slope,
    send_sem, recv_sem, local_sem, hid_send, hid_recv, act_send, act_recv,
):
    row, col, x = lax.axis_index("row"), lax.axis_index("col"), lax.axis_index("dp")
    zh, c = row // 2, row % 2
    y, zl = col // 2, col % 2
    factor = 1.0 / 64.0

    z_right, z_left = {"row": ((zh + 1) % 4) * 2 + c}, {"row": ((zh + 3) % 4) * 2 + c}
    z_across = {"row": ((zh + 2) % 4) * 2 + c}
    y_right, y_left = {"col": ((y + 1) % 4) * 2 + zl}, {"col": ((y + 3) % 4) * 2 + zl}
    x_right, x_left, x_across = {"dp": (x + 1) % 4}, {"dp": (x + 3) % 4}, {"dp": (x + 2) % 4}
    twin = {"row": zh * 2 + 1 - c}
    beside = {"col": y * 2 + 1 - zl}
    outer = {"row": ((zh + 3 + 2 * zl) % 4) * 2 + c, "col": y * 2 + 1 - zl}

    locals_ = [
        pltpu.make_async_copy(x_ref, xg.at[zh], local_sem.at[0]),
        pltpu.make_async_copy(u_ref, ug.at[zh], local_sem.at[1]),
        pltpu.make_async_copy(e_ref.at[:, rows_at(zh * 512, 512, 512)], eg.at[zh], local_sem.at[2]),
        pltpu.make_async_copy(c_ref.at[rows_at(zh * 512, 512, 512)], cg.at[zh], local_sem.at[3]),
    ]
    for copy in locals_:
        copy.start()

    barrier = pltpu.get_barrier_semaphore()
    peers = (z_right, z_left, z_across, y_right, y_left, x_right, x_left, x_across, twin, beside, outer)
    for peer in peers:
        pl.semaphore_signal(barrier, inc=1, device_id=peer, device_id_type=MESH)
    pl.semaphore_wait(barrier, len(peers))

    net = Net(send_sem, recv_sem)

    def z_gather(buf, slot):
        return PairRing(
            net, zh, zl, outer, beside, lambda j, first, size: buf.at[j, rows_at(slot * 256 + first, size, 128)]
        )

    def y_gathers(buf, ring):
        def gather(d):
            def at(size, first):
                return lambda j: buf.at[d, rows_at(j * 256 + first, size, 128)]
            return Gather(net, y, y_left, y_right, at(256, 0), at(128, 0), at(128, 128))
        return [gather(d) for d in (ring.early, ring.late, ring.across)]

    def x_gathers(at, order):
        return [
            Gather(net, x, x_left, x_right, at(d, 128, 0), at(d, 64, 0), at(d, 64, 64)) for d in order
        ]

    others = [(zh + d) % 4 for d in (3, 1, 2)]

    def weight_at(buf):
        return lambda d, size, first: lambda j: buf.at[d, rows_at(j * 128 + first, size, 64)]

    def weight_slot(buf):
        return lambda j, first, size: buf.at[j, rows_at(x * 128 + first, size, 64)]

    xz, uz = z_gather(xg, y), z_gather(ug, y)
    xy, uy = y_gathers(xg, xz), y_gathers(ug, uz)
    ez = Exchange(
        net, zh, z_left, z_right,
        lambda j, first, size: e_ref.at[rows_at(x * 128 + first, size, 64), rows_at(j * 512, 512, 512)],
        weight_slot(eg), relay_e, 128,
    )
    cz = Exchange(
        net, zh, z_left, z_right,
        lambda j, first, size: c_ref.at[rows_at(j * 512 + x * 128 + first, size, 64)],
        weight_slot(cg), relay_c, 128,
    )
    ex, cx = x_gathers(weight_at(eg), others), x_gathers(weight_at(cg), others)

    def hid_copy(k, slot):
        return pltpu.make_async_remote_copy(
            part.at[k, slot, 1 - c], got.at[k, slot], hid_send.at[k, slot], hid_recv.at[k, slot],
            device_id=twin, device_id_type=MESH,
        )

    def act_copy(k, slot, half):
        block = ah.at[k, half, rows_at(slot * 256, 256, 256)]
        return pltpu.make_async_remote_copy(
            block, block, act_send.at[k, slot], act_recv.at[k, slot],
            device_id=twin, device_id_type=MESH,
        )

    def forward_part(slot):
        where = rows_at(slot * 256, 256, 256)

        @pl.loop(0, 2)
        def _(half):
            cols = rows_at(half * 256, 256, 256)
            acc = dot(xg[0, where], eg[0, :, cols], NN)
            for j in range(1, 4):
                acc = acc + dot(xg[j, where], eg[j, :, cols], NN)
            part[0, slot, half] = acc

        hid_copy(0, slot).start()

    def back_part(slot):
        where = rows_at(slot * 256, 256, 256)

        @pl.loop(0, 2)
        def _(half):
            cols = rows_at(half * 256, 256, 256)
            acc = dot(ug[0, where], cg[0, cols], NT)
            for j in range(1, 4):
                acc = acc + dot(ug[j, where], cg[j, cols], NT)
            part[1, slot, half] = acc

        hid_copy(1, slot).start()

    def activate(slot):
        hid_copy(0, slot).wait_recv()
        bias = b_ref[row]

        @pl.loop(0, 8)
        def _(r):
            rows = rows_at(r * 32, 32, 32)
            pre = part[0, slot, c, rows] + got[0, slot, rows] + bias
            v = pre.astype(BF).astype(F32)
            k0, k1 = 0.7978845608028654, 0.044715
            sq = v * v
            t = jnp.tanh(k0 * (v + k1 * (sq * v)))
            half = 0.5 * (1.0 + t)
            slope[slot, rows] = half + (0.5 * v) * (1.0 - t * t) * (k0 * (1.0 + 3.0 * k1 * sq))
            ah[0, c, rows_at(slot * 256 + r * 32, 32, 32)] = (v * half).astype(BF)

        act_copy(0, slot, c).start()

    def multiply(slot):
        hid_copy(1, slot).wait_recv()

        @pl.loop(0, 4)
        def _(r):
            rows = rows_at(r * 64, 64, 64)
            back = (part[1, slot, c, rows] + got[1, slot, rows]).astype(BF).astype(F32)
            ah[1, c, rows_at(slot * 256 + r * 64, 64, 64)] = (back * slope[slot, rows]).astype(BF)

        act_copy(1, slot, c).start()

    def swapped(k):
        @pl.loop(0, 4)
        def _(slot):
            act_copy(k, slot, 1 - c).wait_recv()
            hid_copy(k, slot).wait_send()
            act_copy(k, slot, c).wait_send()

    def reduce_to(axis, part_at, inbox, out):
        me, left, right = axis
        return Reduce(net, me, left, right, part_at, inbox, add_into,
                      lambda h, *parts: total_into(out(h), parts))

    over_x, over_y, over_z = (x, x_left, x_right), (y, y_left, y_right), (zh, z_left, z_right)
    e_red = reduce_to(over_x, lambda j, h: ge.at[j, pl.ds(2 * h, 2)], in_e, lambda h: sum_e.at[pl.ds(2 * h, 2)])
    c_red = reduce_to(over_x, lambda j, h: gc.at[j, pl.ds(2 * h, 2)], in_c, lambda h: sum_c.at[pl.ds(2 * h, 2)])

    def own_rows(s, first, size):
        return ox_ref.at[rows_at(y * 256 + s * 128 + zl * 64 + first, size, 32)]

    def per_chunk(s):
        down = reduce_to(over_y, lambda j, h: gx.at[s, j, pl.ds(2 * h, 2)], in_x.at[s],
                         lambda h: sum_x.at[s, pl.ds(2 * h, 2)])
        along = reduce_to(over_z, lambda j, h: pair_sum.at[s, j, pl.ds(32 * h, 32)], in_z.at[s],
                          lambda h: own_rows(s, 32 * h, 32))
        def at(size, first):
            return lambda j: ox_ref.at[rows_at(j * 256 + s * 128 + first, size, 64)]
        spread = Gather(net, y, y_left, y_right, at(128, 0), at(64, 0), at(64, 64))
        return down, along, spread, net.ids(2)

    chunks = [per_chunk(s) for s in range(2)]

    def out_e(j, first, size):
        return oe_ref.at[rows_at(x * 128 + first, size, 64), rows_at(j * 512, 512, 512)]

    def out_c(j, first, size):
        return oc_ref.at[rows_at(j * 512 + x * 128 + first, size, 64)]

    e_swap = Exchange(net, zh, z_left, z_right, lambda j, first, size: sum_e.at[j, pl.ds(first, size)],
                      out_e, relay_ge, 128)
    c_swap = Exchange(net, zh, z_left, z_right, lambda j, first, size: sum_c.at[j, pl.ds(first, size)],
                      out_c, relay_gc, 128)
    order = [zh] + others
    e_out = x_gathers(
        lambda d, size, first: lambda j: oe_ref.at[rows_at(j * 128 + first, size, 64), rows_at(d * 512, 512, 512)],
        order)
    c_out = x_gathers(
        lambda d, size, first: lambda j: oc_ref.at[rows_at(d * 512 + j * 128 + first, size, 64)], order)

    def pair_send(s):
        net.send(chunks[s][3][0], sum_x.at[s, :, rows_at((1 - zl) * 64, 64, 64)], pair_in.at[s], beside)

    def pair_add(s):
        net.arrived(chunks[s][3][0], pair_in.at[s], beside)

        @pl.loop(0, 4)
        def _(j):
            mine = sum_x[s, j, rows_at(zl * 64, 64, 64)].astype(F32)
            pair_sum[s, j] = (mine + pair_in[s, j].astype(F32)).astype(BF)

    def pair_back(s):
        net.send(chunks[s][3][1], own_rows(s, 0, 64), own_rows(s, 0, 64), beside)

    def pair_got(s):
        there = ox_ref.at[rows_at(y * 256 + s * 128 + (1 - zl) * 64, 64, 64)]
        net.arrived(chunks[s][3][1], there, beside)

    small_k = net.ids(6)

    def grad_expand():
        @pl.loop(0, 4)
        def _(j):
            for h in range(2):
                acc = (dot(xg[j], ah[1, h], TN) * factor).astype(BF)
                for q in range(4):
                    ge[q, j, :, pl.ds(h * 256, 256)] = acc[q * 128:(q + 1) * 128]

    def grad_contract():
        @pl.loop(0, 4)
        def _(j):
            for h in range(2):
                acc = (dot(ah[0, h], ug[j], TN) * factor).astype(BF)
                gc[2 * h, j] = acc[:128]
                gc[2 * h + 1, j] = acc[128:]

    def grad_tokens(s):
        @pl.loop(0, 4)
        def _(j):
            first = ah[1, 0].reshape(4, 2, 128, 256)[:, s].reshape(512, 256)
            second = ah[1, 1].reshape(4, 2, 128, 256)[:, s].reshape(512, 256)
            acc = dot(first, eg[j, :, pl.ds(0, 256)], NT) + dot(second, eg[j, :, pl.ds(256, 256)], NT)
            acc = acc.astype(BF)
            for slot in range(4):
                gx[s, slot, j] = acc[slot * 128:(slot + 1) * 128]

    def token_sums():
        for h in range(2):
            def add_rows(n, acc):
                block = ah[1, h, rows_at(n * 64, 64, 64)].astype(F32)
                return acc + jnp.sum(block.reshape(8, 8, 256), axis=0)
            acc = lax.fori_loop(0, 16, add_rows, jnp.zeros((8, 256), F32))
            acc = jnp.sum(acc, axis=0, keepdims=True) * factor
            small[pl.ds(0, 8), pl.ds(h * 256, 256)] = jnp.broadcast_to(acc.astype(BF).astype(F32), (8, 256))

        def add_up(n, acc):
            block = ug[zh, rows_at(n * 64, 64, 64)].astype(F32)
            return acc + jnp.sum(block.reshape(8, 8, 512), axis=0)
        acc = lax.fori_loop(0, 16, add_up, jnp.zeros((8, 512), F32))
        acc = jnp.sum(acc, axis=0, keepdims=True) * factor
        small[pl.ds(8, 8)] = jnp.broadcast_to(acc.astype(BF).astype(F32), (8, 512))
        for n, peer in enumerate((x_right, x_left, x_across)):
            net.send(small_k[n], small, small_in.at[n], peer)

    def small_sums():
        for n, peer in enumerate((x_left, x_right, x_across)):
            net.arrived(small_k[n], small_in.at[n], peer)
        whole = ((small[...] + small_in[0]) + small_in[1]) + small_in[2]
        ob_ref[zh] = whole[:8]
        oo_ref[...] = whole[8:]
        for n, peer in enumerate((z_right, z_left, z_across)):
            net.send(small_k[3 + n], ob_ref.at[zh], ob_ref.at[zh], peer)

    locals_[0].wait()
    xz.start()
    locals_[1].wait()
    uz.start()
    xz.get_early()
    xy[0].start()
    uz.get_early()
    uy[0].start()
    xz.get_late()
    xy[1].start()
    ez.start()
    xz.get_across()
    uy[0].forward()
    ez.forward()
    uz.get_late()
    uy[1].start()
    cz.start()
    xy[1].forward()
    ez.near()
    ex[0].start()
    ex[1].start()
    xz.finish()
    xy[2].start()
    xy[0].forward()
    ez.finish()
    ex[2].start()
    ex[0].forward()
    ex[1].forward()
    uz.get_across()
    ex[2].forward()
    xy[2].forward()
    cz.near()
    cx[0].start()
    cx[1].start()
    cz.forward()
    locals_[2].wait()
    for gather in ex:
        gather.finish()
    uz.finish()
    uy[2].start()
    uy[1].forward()
    forward_part((y + 1) % 4)
    forward_part(y)
    forward_part((y + 3) % 4)
    for gather in xy:
        gather.finish()
    forward_part((y + 2) % 4)
    cz.finish()
    cx[2].start()
    activate(y)
    cx[0].forward()
    cx[1].forward()
    activate((y + 2) % 4)
    uy[2].forward()
    activate((y + 1) % 4)
    activate((y + 3) % 4)
    cx[2].forward()
    locals_[3].wait()
    for gather in cx:
        gather.finish()
    swapped(0)
    for gather in uy:
        gather.finish()
    back_part((y + 2) % 4)
    grad_contract()
    c_red.far()
    back_part((y + 1) % 4)
    back_part((y + 3) % 4)
    back_part(y)
    multiply((y + 1) % 4)
    multiply(y)
    multiply((y + 3) % 4)
    c_red.near()
    multiply((y + 2) % 4)
    swapped(1)
    grad_tokens(1)
    chunks[1][0].far()
    c_red.join()
    grad_tokens(0)
    chunks[1][0].near()
    grad_expand()
    e_red.far()
    chunks[1][0].join()
    e_red.near()
    chunks[0][0].far()
    c_red.finish()
    oc_ref[rows_at(zh * 512 + x * 128, 128, 128)] = sum_c[zh]
    c_swap.start()
    c_swap.forward()
    chunks[0][0].near()
    e_red.join()
    chunks[1][0].finish()
    pair_send(1)
    c_swap.finish()
    c_out[3].start()
    c_out[0].start()
    e_red.finish()
    oe_ref[rows_at(x * 128, 128, 128), rows_at(zh * 512, 512, 512)] = sum_e[zh]
    e_swap.start()
    chunks[0][0].join()
    pair_add(1)
    chunks[1][1].far()
    chunks[1][1].near()
    c_swap.near()
    c_out[1].start()
    c_out[2].start()
    chunks[0][0].finish()
    pair_send(0)
    token_sums()
    e_out[0].start()
    e_swap.near()
    e_out[1].start()
    e_out[2].start()
    e_out[0].forward()
    chunks[1][1].join()
    pair_add(0)
    chunks[0][1].far()
    chunks[0][1].near()
    e_out[1].forward()
    chunks[1][1].finish()
    pair_back(1)
    chunks[0][1].join()
    e_swap.forward()
    e_out[2].forward()
    c_out[2].forward()
    chunks[0][1].finish()
    pair_back(0)
    c_out[1].forward()
    pair_got(1)
    chunks[1][2].start()
    e_swap.finish()
    e_out[3].start()
    small_sums()
    c_out[3].forward()
    c_out[0].forward()
    pair_got(0)
    chunks[0][2].start()
    chunks[1][2].forward()
    e_out[3].forward()
    chunks[0][2].forward()
    for gather in e_out + c_out:
        gather.finish()
    for chunk in chunks:
        chunk[2].finish()
    for n, d in enumerate((3, 1, 2)):
        net.arrived(small_k[3 + n], ob_ref.at[(zh + d) % 4], z_across)
    net.drain()
    assert net.used <= 224


def finish(ox, oe, ob, oc, oo, gx, ge, gb, gc, go, tall, wide, sem):
    copies = [
        pltpu.make_async_copy(src, dst, sem.at[k]) for k, (src, dst) in enumerate(((oe, ge), (oc, gc), (ox, gx)))
    ]
    for copy in copies:
        copy.start()
    for k in range(4):
        cols = pl.ds(k * 128, 128)
        for j in range(4):
            tall[pl.ds(j * 4 + k, 1)] = ob[j, pl.ds(0, 1), cols]
        wide[pl.ds(k, 1)] = oo[pl.ds(0, 1), cols]
    gb[...] = tall[...].astype(BF)
    go[...] = wide[...].astype(BF)
    for copy in copies:
        copy.wait()


def local(inputs, upstream, expand, biases, contract):
    vmem = pl.BlockSpec(memory_space=pltpu.VMEM)
    anywhere = pl.BlockSpec(memory_space=pl.ANY)
    dma = pltpu.SemaphoreType.DMA
    ox, oe, ob, oc, oo = pl.pallas_call(
        kernel,
        out_shape=(
            pltpu.VMEM((1024, 512), BF),
            pltpu.VMEM((512, 2048), BF),
            pltpu.VMEM((4, 8, 512), F32),
            pltpu.VMEM((2048, 512), BF),
            pltpu.VMEM((8, 512), F32),
        ),
        in_specs=[anywhere, anywhere, anywhere, vmem, anywhere],
        out_specs=(vmem, vmem, vmem, vmem, vmem),
        scratch_shapes=[
            pltpu.VMEM((4, 1024, 512), BF),
            pltpu.VMEM((4, 1024, 512), BF),
            pltpu.VMEM((4, 512, 512), BF),
            pltpu.VMEM((4, 512, 512), BF),
            pltpu.VMEM((2, 4, 2, 256, 256), F32),
            pltpu.VMEM((2, 4, 256, 256), F32),
            pltpu.VMEM((2, 2, 1024, 256), BF),
            pltpu.VMEM((2, 64, 512), BF),
            pltpu.VMEM((2, 64, 512), BF),
            pltpu.VMEM((4, 4, 128, 512), BF),
            pltpu.VMEM((4, 4, 128, 512), BF),
            pltpu.VMEM((2, 4, 4, 128, 512), BF),
            pltpu.VMEM((6, 2, 128, 512), BF),
            pltpu.VMEM((6, 2, 128, 512), BF),
            pltpu.VMEM((2, 6, 2, 128, 512), BF),
            pltpu.VMEM((4, 128, 512), BF),
            pltpu.VMEM((4, 128, 512), BF),
            pltpu.VMEM((2, 4, 128, 512), BF),
            pltpu.VMEM((2, 64, 512), BF),
            pltpu.VMEM((2, 64, 512), BF),
            pltpu.VMEM((2, 4, 64, 512), BF),
            pltpu.VMEM((2, 4, 64, 512), BF),
            pltpu.VMEM((2, 6, 32, 512), BF),
            pltpu.VMEM((16, 512), F32),
            pltpu.VMEM((3, 16, 512), F32),
            pltpu.VMEM((4, 256, 256), F32),
            dma((224,)),
            dma((224,)),
            dma((4,)),
            dma((2, 4)),
            dma((2, 4)),
            dma((2, 4)),
            dma((2, 4)),
        ],
        compiler_params=pltpu.CompilerParams(
            collective_id=0, has_side_effects=True, vmem_limit_bytes=50 * 1024 * 1024
        ),
    )(inputs, upstream, expand, biases.reshape(8, 1, 256), contract)
    gx, ge, gb, gc, go = pl.pallas_call(
        finish,
        out_shape=(
            jax.ShapeDtypeStruct((1024, 512), BF),
            jax.ShapeDtypeStruct((512, 2048), BF),
            jax.ShapeDtypeStruct((16, 128), BF),
            jax.ShapeDtypeStruct((2048, 512), BF),
            jax.ShapeDtypeStruct((4, 128), BF),
        ),
        in_specs=[vmem] * 5,
        out_specs=(anywhere, anywhere, vmem, anywhere, vmem),
        scratch_shapes=[pltpu.VMEM((16, 128), F32), pltpu.VMEM((4, 128), F32), dma((3,))],
        compiler_params=pltpu.CompilerParams(vmem_limit_bytes=12 * 1024 * 1024),
    )(ox, oe, ob, oc, oo)
    return gx, ge, gb.reshape(2048), gc, go.reshape(512)


def solution(mesh):
    in_specs = (P("dp", "row"), P("dp", "row"), P("row", "col"), P("col"), P("col", "row"))
    out_specs = (P("dp", "row"), P("row", "col"), P("col"), P("col", "row"), P("row"))
    return jax.shard_map(local, mesh=mesh, in_specs=in_specs, out_specs=out_specs, check_vma=False)
```

```python
import functools

import jax
import jax.numpy as jnp
from jax import lax
from jax.experimental import pallas as pl
from jax.experimental.pallas import tpu as pltpu
from jax.sharding import PartitionSpec as P

BF = jnp.bfloat16
F32 = jnp.float32
MESH = pl.DeviceIdType.MESH
NN = (((1,), (0,)), ((), ()))
NT = (((1,), (1,)), ((), ()))
TN = (((0,), (0,)), ((), ()))


def dot(a, b, dims):
    return lax.dot_general(a, b, dims, preferred_element_type=F32)


class Net:
    def __init__(self, send_sem, recv_sem):
        self.send_sem, self.recv_sem = send_sem, recv_sem
        self.used, self.sent = 0, []

    def ids(self, count):
        first = self.used
        self.used += count
        return range(first, first + count)

    def send(self, k, src, dst, device):
        copy = pltpu.make_async_remote_copy(
            src, dst, self.send_sem.at[k], self.recv_sem.at[k], device_id=device, device_id_type=MESH
        )
        copy.start()
        self.sent.append(copy)

    def arrived(self, k, dst, device):
        pltpu.make_async_remote_copy(
            dst, dst, self.send_sem.at[k], self.recv_sem.at[k], device_id=device, device_id_type=MESH
        ).wait_recv()

    def drain(self):
        for copy in self.sent:
            copy.wait_send()


class Gather:
    def __init__(self, net, me, left, right, full, top, bottom):
        self.net, self.me, self.left, self.right = net, me, left, right
        self.full, self.top, self.bottom = full, top, bottom
        self.k = net.ids(4)

    def start(self):
        block = self.full(self.me)
        self.net.send(self.k[0], block, block, self.right)
        self.net.send(self.k[1], block, block, self.left)

    def near(self):
        self.net.arrived(self.k[0], self.full((self.me + 3) % 4), self.left)
        self.net.arrived(self.k[1], self.full((self.me + 1) % 4), self.right)

    def forward(self):
        before, after = (self.me + 3) % 4, (self.me + 1) % 4
        self.net.arrived(self.k[0], self.full(before), self.left)
        self.net.send(self.k[2], self.top(before), self.top(before), self.right)
        self.net.arrived(self.k[1], self.full(after), self.right)
        self.net.send(self.k[3], self.bottom(after), self.bottom(after), self.left)

    def finish(self):
        across = (self.me + 2) % 4
        self.net.arrived(self.k[2], self.top(across), self.left)
        self.net.arrived(self.k[3], self.bottom(across), self.right)


class Exchange:
    def __init__(self, net, me, left, right, src, dst, relay, rows):
        self.net, self.me, self.left, self.right = net, me, left, right
        self.src, self.dst, self.relay, self.rows = src, dst, relay, rows
        self.k = net.ids(6)

    def start(self):
        me, half = self.me, self.rows // 2
        before, after, across = (me + 3) % 4, (me + 1) % 4, (me + 2) % 4
        self.net.send(self.k[2], self.src(across, 0, half), self.relay.at[0], self.right)
        self.net.send(self.k[3], self.src(across, half, half), self.relay.at[1], self.left)
        self.net.send(self.k[0], self.src(after, 0, self.rows), self.dst(me, 0, self.rows), self.right)
        self.net.send(self.k[1], self.src(before, 0, self.rows), self.dst(me, 0, self.rows), self.left)

    def forward(self):
        me, half = self.me, self.rows // 2
        before, after = (me + 3) % 4, (me + 1) % 4
        self.net.arrived(self.k[2], self.relay.at[0], self.left)
        self.net.send(self.k[4], self.relay.at[0], self.dst(before, 0, half), self.right)
        self.net.arrived(self.k[3], self.relay.at[1], self.right)
        self.net.send(self.k[5], self.relay.at[1], self.dst(after, half, half), self.left)

    def near(self):
        me = self.me
        self.net.arrived(self.k[0], self.dst((me + 3) % 4, 0, self.rows), self.left)
        self.net.arrived(self.k[1], self.dst((me + 1) % 4, 0, self.rows), self.right)

    def finish(self):
        half, across = self.rows // 2, (self.me + 2) % 4
        self.net.arrived(self.k[4], self.dst(across, 0, half), self.left)
        self.net.arrived(self.k[5], self.dst(across, half, half), self.right)


class Reduce:
    def __init__(self, net, me, left, right, part, inbox, add, total):
        self.net, self.me, self.left, self.right = net, me, left, right
        self.part, self.inbox, self.add, self.total = part, inbox, add, total
        self.k = net.ids(6)

    def far(self):
        across = (self.me + 2) % 4
        self.net.send(self.k[0], self.part(across, 0), self.inbox.at[0], self.right)
        self.net.send(self.k[1], self.part(across, 1), self.inbox.at[1], self.left)

    def near(self):
        before, after = (self.me + 3) % 4, (self.me + 1) % 4
        self.net.send(self.k[2], self.part(after, 1), self.inbox.at[2], self.right)
        self.net.send(self.k[3], self.part(before, 0), self.inbox.at[3], self.left)

    def join(self):
        before, after = (self.me + 3) % 4, (self.me + 1) % 4
        self.net.arrived(self.k[0], self.inbox.at[0], self.left)
        self.add(self.part(after, 0), self.inbox.at[0])
        self.net.send(self.k[4], self.part(after, 0), self.inbox.at[4], self.right)
        self.net.arrived(self.k[1], self.inbox.at[1], self.right)
        self.add(self.part(before, 1), self.inbox.at[1])
        self.net.send(self.k[5], self.part(before, 1), self.inbox.at[5], self.left)

    def finish(self):
        self.net.arrived(self.k[3], self.inbox.at[3], self.right)
        self.net.arrived(self.k[4], self.inbox.at[4], self.left)
        self.total(0, self.part(self.me, 0), self.inbox.at[3], self.inbox.at[4])
        self.net.arrived(self.k[2], self.inbox.at[2], self.left)
        self.net.arrived(self.k[5], self.inbox.at[5], self.right)
        self.total(1, self.part(self.me, 1), self.inbox.at[2], self.inbox.at[5])


def add_into(target, other):
    rows = min(64, target.shape[-2])
    lead = target.shape[0] if len(target.shape) == 3 else 1
    depth = target.shape[-2]

    def view(ref, i, r):
        where = pl.ds(pl.multiple_of(r * rows, rows), rows)
        return ref.at[i, where] if len(ref.shape) == 3 else ref.at[where]

    @pl.loop(0, lead * (depth // rows))
    def _(n):
        i, r = n // (depth // rows), n % (depth // rows)
        mine = view(target, i, r)
        mine[...] = (mine[...].astype(F32) + view(other, i, r)[...].astype(F32)).astype(BF)


def total_into(out, parts):
    rows = min(64, out.shape[-2])
    lead = out.shape[0] if len(out.shape) == 3 else 1
    depth = out.shape[-2]

    def view(ref, i, r):
        where = pl.ds(pl.multiple_of(r * rows, rows), rows)
        return ref.at[i, where] if len(ref.shape) == 3 else ref.at[where]

    @pl.loop(0, lead * (depth // rows))
    def _(n):
        i, r = n // (depth // rows), n % (depth // rows)
        acc = view(parts[0], i, r)[...].astype(F32)
        for other in parts[1:]:
            acc = acc + view(other, i, r)[...].astype(F32)
        view(out, i, r)[...] = acc.astype(BF)


def rows_at(start, size, unit):
    return pl.ds(pl.multiple_of(start, unit), size)


class PairRing:
    def __init__(self, net, zh, zl, outer, inner, block):
        self.net, self.outer, self.inner, self.block = net, outer, inner, block
        self.own, self.across = zh, (zh + 2) % 4
        self.early, self.late = (zh + 3 + 2 * zl) % 4, (zh + 5 - 2 * zl) % 4
        self.out_half, self.in_half = (1 - zl) * 128, zl * 128
        self.k = net.ids(4)

    def send(self, k, block, device):
        self.net.send(self.k[k], block, block, device)

    def start(self):
        self.send(0, self.block(self.own, 0, 256), self.outer)

    def get_early(self):
        block = self.block(self.early, 0, 256)
        self.net.arrived(self.k[0], block, self.outer)
        self.send(1, block, self.inner)

    def get_late(self):
        self.net.arrived(self.k[1], self.block(self.late, 0, 256), self.inner)
        self.send(2, self.block(self.late, self.out_half, 128), self.outer)

    def get_across(self):
        block = self.block(self.across, self.in_half, 128)
        self.net.arrived(self.k[2], block, self.outer)
        self.send(3, block, self.inner)

    def finish(self):
        self.net.arrived(self.k[3], self.block(self.across, self.out_half, 128), self.inner)


def kernel(
    x_ref, u_ref, e_ref, b_ref, c_ref,
    ox_ref, oe_ref, ob_ref, oc_ref, oo_ref,
    xg, ug, eg, cg, part, got, ah, relay_e, relay_c,
    ge, gc, gx, in_e, in_c, in_x, sum_e, sum_c, sum_x, relay_ge, relay_gc,
    pair_in, pair_sum, in_z, small, small_in, slope,
    send_sem, recv_sem, local_sem, hid_send, hid_recv, act_send, act_recv,
):
    row, col, x = lax.axis_index("row"), lax.axis_index("col"), lax.axis_index("dp")
    zh, c = row // 2, row % 2
    y, zl = col // 2, col % 2
    factor = 1.0 / 64.0

    z_right, z_left = {"row": ((zh + 1) % 4) * 2 + c}, {"row": ((zh + 3) % 4) * 2 + c}
    y_right, y_left = {"col": ((y + 1) % 4) * 2 + zl}, {"col": ((y + 3) % 4) * 2 + zl}
    x_right, x_left, x_across = {"dp": (x + 1) % 4}, {"dp": (x + 3) % 4}, {"dp": (x + 2) % 4}
    twin = {"row": zh * 2 + 1 - c}
    beside = {"col": y * 2 + 1 - zl}
    outer = {"row": ((zh + 3 + 2 * zl) % 4) * 2 + c, "col": y * 2 + 1 - zl}

    locals_ = [
        pltpu.make_async_copy(x_ref, xg.at[zh], local_sem.at[0]),
        pltpu.make_async_copy(u_ref, ug.at[zh], local_sem.at[1]),
        pltpu.make_async_copy(e_ref.at[:, rows_at(zh * 512, 512, 512)], eg.at[zh], local_sem.at[2]),
        pltpu.make_async_copy(c_ref.at[rows_at(zh * 512, 512, 512)], cg.at[zh], local_sem.at[3]),
    ]
    for copy in locals_:
        copy.start()

    barrier = pltpu.get_barrier_semaphore()
    peers = (z_right, z_left, y_right, y_left, x_right, x_left, x_across, twin, beside, outer)
    for peer in peers:
        pl.semaphore_signal(barrier, inc=1, device_id=peer, device_id_type=MESH)
    pl.semaphore_wait(barrier, len(peers))

    net = Net(send_sem, recv_sem)

    def z_gather(buf, slot):
        return PairRing(
            net, zh, zl, outer, beside, lambda j, first, size: buf.at[j, rows_at(slot * 256 + first, size, 128)]
        )

    def y_gathers(buf, ring):
        def gather(d):
            def at(size, first):
                return lambda j: buf.at[d, rows_at(j * 256 + first, size, 128)]
            return Gather(net, y, y_left, y_right, at(256, 0), at(128, 0), at(128, 128))
        return [gather(d) for d in (ring.early, ring.late, ring.across)]

    def x_gathers(at, order):
        return [
            Gather(net, x, x_left, x_right, at(d, 128, 0), at(d, 64, 0), at(d, 64, 64)) for d in order
        ]

    others = [(zh + d) % 4 for d in (3, 1, 2)]

    def weight_at(buf):
        return lambda d, size, first: lambda j: buf.at[d, rows_at(j * 128 + first, size, 64)]

    def weight_slot(buf):
        return lambda j, first, size: buf.at[j, rows_at(x * 128 + first, size, 64)]

    xz, uz = z_gather(xg, y), z_gather(ug, y)
    xy, uy = y_gathers(xg, xz), y_gathers(ug, uz)
    ez = Exchange(
        net, zh, z_left, z_right,
        lambda j, first, size: e_ref.at[rows_at(x * 128 + first, size, 64), rows_at(j * 512, 512, 512)],
        weight_slot(eg), relay_e, 128,
    )
    cz = Exchange(
        net, zh, z_left, z_right,
        lambda j, first, size: c_ref.at[rows_at(j * 512 + x * 128 + first, size, 64)],
        weight_slot(cg), relay_c, 128,
    )
    ex, cx = x_gathers(weight_at(eg), others), x_gathers(weight_at(cg), others)

    def hid_copy(k, slot):
        return pltpu.make_async_remote_copy(
            part.at[k, slot, 1 - c], got.at[k, slot], hid_send.at[k, slot], hid_recv.at[k, slot],
            device_id=twin, device_id_type=MESH,
        )

    def act_copy(k, slot, half):
        block = ah.at[k, half, rows_at(slot * 256, 256, 256)]
        return pltpu.make_async_remote_copy(
            block, block, act_send.at[k, slot], act_recv.at[k, slot],
            device_id=twin, device_id_type=MESH,
        )

    def forward_part(slot):
        where = rows_at(slot * 256, 256, 256)

        @pl.loop(0, 2)
        def _(half):
            cols = rows_at(half * 256, 256, 256)
            acc = dot(xg[0, where], eg[0, :, cols], NN)
            for j in range(1, 4):
                acc = acc + dot(xg[j, where], eg[j, :, cols], NN)
            part[0, slot, half] = acc

        hid_copy(0, slot).start()

    def back_half(half):
        cols = rows_at(half * 256, 256, 256)

        @pl.loop(0, 2)
        def _(n):
            where = rows_at(n * 512, 512, 512)
            acc = dot(ug[0, where], cg[0, cols], NT)
            for j in range(1, 4):
                acc = acc + dot(ug[j, where], cg[j, cols], NT)
            part[1, 2 * n, half] = acc[:256]
            part[1, 2 * n + 1, half] = acc[256:]

    def back_theirs():
        back_half(1 - c)

        @pl.loop(0, 4)
        def _(slot):
            hid_copy(1, slot).start()

    def activate(slot):
        hid_copy(0, slot).wait_recv()
        bias = b_ref[row]

        @pl.loop(0, 8)
        def _(r):
            rows = rows_at(r * 32, 32, 32)
            pre = part[0, slot, c, rows] + got[0, slot, rows] + bias
            v = pre.astype(BF).astype(F32)
            k0, k1 = 0.7978845608028654, 0.044715
            sq = v * v
            t = jnp.tanh(k0 * (v + k1 * (sq * v)))
            half = 0.5 * (1.0 + t)
            slope[slot, rows] = half + (0.5 * v) * (1.0 - t * t) * (k0 * (1.0 + 3.0 * k1 * sq))
            ah[0, c, rows_at(slot * 256 + r * 32, 32, 32)] = (v * half).astype(BF)

        act_copy(0, slot, c).start()

    def multiply(slot):
        hid_copy(1, slot).wait_recv()

        @pl.loop(0, 4)
        def _(r):
            rows = rows_at(r * 64, 64, 64)
            back = (part[1, slot, c, rows] + got[1, slot, rows]).astype(BF).astype(F32)
            ah[1, c, rows_at(slot * 256 + r * 64, 64, 64)] = (back * slope[slot, rows]).astype(BF)

        act_copy(1, slot, c).start()

    def swapped(k):
        @pl.loop(0, 4)
        def _(slot):
            act_copy(k, slot, 1 - c).wait_recv()
            hid_copy(k, slot).wait_send()
            act_copy(k, slot, c).wait_send()

    def reduce_to(axis, part_at, inbox, out):
        me, left, right = axis
        return Reduce(net, me, left, right, part_at, inbox, add_into,
                      lambda h, *parts: total_into(out(h), parts))

    over_x, over_y, over_z = (x, x_left, x_right), (y, y_left, y_right), (zh, z_left, z_right)
    e_red = reduce_to(over_x, lambda j, h: ge.at[j, pl.ds(2 * h, 2)], in_e, lambda h: sum_e.at[pl.ds(2 * h, 2)])
    c_red = reduce_to(over_x, lambda j, h: gc.at[j, pl.ds(2 * h, 2)], in_c, lambda h: sum_c.at[pl.ds(2 * h, 2)])

    def own_rows(s, first, size):
        return ox_ref.at[rows_at(y * 256 + s * 128 + zl * 64 + first, size, 32)]

    def per_chunk(s):
        down = reduce_to(over_y, lambda j, h: gx.at[s, j, pl.ds(2 * h, 2)], in_x.at[s],
                         lambda h: sum_x.at[s, pl.ds(2 * h, 2)])
        along = reduce_to(over_z, lambda j, h: pair_sum.at[s, j, pl.ds(32 * h, 32)], in_z.at[s],
                          lambda h: own_rows(s, 32 * h, 32))
        def at(size, first):
            return lambda j: ox_ref.at[rows_at(j * 256 + s * 128 + first, size, 64)]
        spread = Gather(net, y, y_left, y_right, at(128, 0), at(64, 0), at(64, 64))
        return down, along, spread, net.ids(2)

    chunks = [per_chunk(s) for s in range(2)]

    def out_e(j, first, size):
        return oe_ref.at[rows_at(x * 128 + first, size, 64), rows_at(j * 512, 512, 512)]

    def out_c(j, first, size):
        return oc_ref.at[rows_at(j * 512 + x * 128 + first, size, 64)]

    e_swap = Exchange(net, zh, z_left, z_right, lambda j, first, size: sum_e.at[j, pl.ds(first, size)],
                      out_e, relay_ge, 128)
    c_swap = Exchange(net, zh, z_left, z_right, lambda j, first, size: sum_c.at[j, pl.ds(first, size)],
                      out_c, relay_gc, 128)
    order = [zh] + others
    e_out = x_gathers(
        lambda d, size, first: lambda j: oe_ref.at[rows_at(j * 128 + first, size, 64), rows_at(d * 512, 512, 512)],
        order)
    c_out = x_gathers(
        lambda d, size, first: lambda j: oc_ref.at[rows_at(d * 512 + j * 128 + first, size, 64)], order)

    def pair_send(s):
        net.send(chunks[s][3][0], sum_x.at[s, :, rows_at((1 - zl) * 64, 64, 64)], pair_in.at[s], beside)

    def pair_add(s):
        net.arrived(chunks[s][3][0], pair_in.at[s], beside)

        @pl.loop(0, 4)
        def _(j):
            mine = sum_x[s, j, rows_at(zl * 64, 64, 64)].astype(F32)
            pair_sum[s, j] = (mine + pair_in[s, j].astype(F32)).astype(BF)

    def pair_back(s):
        net.send(chunks[s][3][1], own_rows(s, 0, 64), own_rows(s, 0, 64), beside)

    def pair_got(s):
        there = ox_ref.at[rows_at(y * 256 + s * 128 + (1 - zl) * 64, 64, 64)]
        net.arrived(chunks[s][3][1], there, beside)

    small_k = net.ids(6)

    def grad_expand():
        @pl.loop(0, 4)
        def _(j):
            for h in range(2):
                acc = (dot(xg[j], ah[1, h], TN) * factor).astype(BF)
                for q in range(4):
                    ge[q, j, :, pl.ds(h * 256, 256)] = acc[q * 128:(q + 1) * 128]

    def grad_contract():
        @pl.loop(0, 4)
        def _(j):
            for h in range(2):
                acc = (dot(ah[0, h], ug[j], TN) * factor).astype(BF)
                gc[2 * h, j] = acc[:128]
                gc[2 * h + 1, j] = acc[128:]

    def grad_tokens(s):
        @pl.loop(0, 4)
        def _(j):
            first = ah[1, 0].reshape(4, 2, 128, 256)[:, s].reshape(512, 256)
            second = ah[1, 1].reshape(4, 2, 128, 256)[:, s].reshape(512, 256)
            acc = dot(first, eg[j, :, pl.ds(0, 256)], NT) + dot(second, eg[j, :, pl.ds(256, 256)], NT)
            acc = acc.astype(BF)
            for slot in range(4):
                gx[s, slot, j] = acc[slot * 128:(slot + 1) * 128]

    def token_sums():
        for h in range(2):
            def add_rows(n, acc):
                block = ah[1, h, rows_at(n * 64, 64, 64)].astype(F32)
                return acc + jnp.sum(block.reshape(8, 8, 256), axis=0)
            acc = lax.fori_loop(0, 16, add_rows, jnp.zeros((8, 256), F32))
            acc = jnp.sum(acc, axis=0, keepdims=True) * factor
            small[pl.ds(0, 8), pl.ds(h * 256, 256)] = jnp.broadcast_to(acc.astype(BF).astype(F32), (8, 256))

        def add_up(n, acc):
            block = ug[zh, rows_at(n * 64, 64, 64)].astype(F32)
            return acc + jnp.sum(block.reshape(8, 8, 512), axis=0)
        acc = lax.fori_loop(0, 16, add_up, jnp.zeros((8, 512), F32))
        acc = jnp.sum(acc, axis=0, keepdims=True) * factor
        small[pl.ds(8, 8)] = jnp.broadcast_to(acc.astype(BF).astype(F32), (8, 512))
        for n, peer in enumerate((x_right, x_left, x_across)):
            net.send(small_k[n], small, small_in.at[n], peer)

    def small_sums():
        for n, peer in enumerate((x_left, x_right, x_across)):
            net.arrived(small_k[n], small_in.at[n], peer)
        whole = ((small[...] + small_in[0]) + small_in[1]) + small_in[2]
        ob_ref[zh] = whole[:8]
        oo_ref[...] = whole[8:]
        for n, peer in enumerate((z_right, z_left)):
            net.send(small_k[3 + n], ob_ref.at[zh], ob_ref.at[zh], peer)

    def small_forward():
        before = ob_ref.at[(zh + 3) % 4]
        net.arrived(small_k[3], before, z_left)
        net.send(small_k[5], before, before, z_right)

    locals_[0].wait()
    xz.start()
    locals_[1].wait()
    uz.start()
    xz.get_early()
    xy[0].start()
    uz.get_early()
    uy[0].start()
    xz.get_late()
    xy[1].start()
    xy[0].forward()
    ez.start()
    uz.get_late()
    uy[1].start()
    xz.get_across()
    xy[1].forward()
    ez.forward()
    ez.near()
    ex[0].start()
    ex[1].start()
    cz.start()
    xz.finish()
    xy[2].start()
    uy[1].forward()
    uz.get_across()
    ez.finish()
    ex[2].start()
    ex[0].forward()
    ex[1].forward()
    ex[2].forward()
    xy[2].forward()
    cz.near()
    cx[0].start()
    cx[1].start()
    cz.forward()
    locals_[2].wait()
    for gather in ex:
        gather.finish()
    uz.finish()
    uy[2].start()
    uy[0].forward()
    forward_part(y)
    forward_part((y + 3) % 4)
    cz.finish()
    cx[2].start()
    forward_part((y + 1) % 4)
    activate((y + 3) % 4)
    cx[0].forward()
    cx[1].forward()
    for gather in xy:
        gather.finish()
    forward_part((y + 2) % 4)
    uy[2].forward()
    cx[2].forward()
    activate((y + 2) % 4)
    activate(y)
    activate((y + 1) % 4)
    swapped(0)
    locals_[3].wait()
    for gather in cx:
        gather.finish()
    for gather in uy:
        gather.finish()
    back_theirs()
    grad_contract()
    c_red.far()
    back_half(c)
    multiply((y + 2) % 4)
    multiply((y + 3) % 4)
    multiply(y)
    c_red.near()
    multiply((y + 1) % 4)
    swapped(1)
    grad_tokens(1)
    chunks[1][0].far()
    chunks[1][0].near()
    c_red.join()
    grad_expand()
    chunks[1][0].join()
    e_red.far()
    grad_tokens(0)
    chunks[0][0].far()
    chunks[0][0].near()
    e_red.near()
    c_red.finish()
    oc_ref[rows_at(zh * 512 + x * 128, 128, 128)] = sum_c[zh]
    c_swap.start()
    c_swap.forward()
    e_red.join()
    c_out[0].start()
    chunks[1][0].finish()
    pair_send(1)
    chunks[0][0].join()
    e_red.finish()
    oe_ref[rows_at(x * 128, 128, 128), rows_at(zh * 512, 512, 512)] = sum_e[zh]
    e_swap.start()
    e_out[0].start()
    token_sums()
    pair_add(1)
    chunks[1][1].far()
    chunks[1][1].near()
    chunks[0][0].finish()
    pair_send(0)
    c_swap.near()
    c_out[1].start()
    c_out[2].start()
    c_swap.finish()
    c_out[3].start()
    c_out[1].forward()
    c_out[3].forward()
    chunks[1][1].join()
    c_out[0].forward()
    e_swap.near()
    e_out[1].start()
    e_out[2].start()
    e_out[0].forward()
    c_out[2].forward()
    pair_add(0)
    chunks[0][1].far()
    chunks[0][1].near()
    chunks[1][1].finish()
    pair_back(1)
    chunks[0][1].join()
    e_out[1].forward()
    e_swap.forward()
    chunks[0][1].finish()
    pair_back(0)
    pair_got(1)
    chunks[1][2].start()
    e_swap.finish()
    e_out[3].start()
    e_out[2].forward()
    small_sums()
    pair_got(0)
    chunks[0][2].start()
    chunks[1][2].forward()
    e_out[3].forward()
    small_forward()
    chunks[0][2].forward()
    for gather in e_out + c_out:
        gather.finish()
    for chunk in chunks:
        chunk[2].finish()
    net.arrived(small_k[4], ob_ref.at[(zh + 1) % 4], z_right)
    net.arrived(small_k[5], ob_ref.at[(zh + 2) % 4], z_left)
    net.drain()
    assert net.used <= 224


def finish(ox, oe, ob, oc, oo, gx, ge, gb, gc, go, tall, wide, sem):
    copies = [
        pltpu.make_async_copy(src, dst, sem.at[k]) for k, (src, dst) in enumerate(((oe, ge), (oc, gc), (ox, gx)))
    ]
    for copy in copies:
        copy.start()
    for k in range(4):
        cols = pl.ds(k * 128, 128)
        for j in range(4):
            tall[pl.ds(j * 4 + k, 1)] = ob[j, pl.ds(0, 1), cols]
        wide[pl.ds(k, 1)] = oo[pl.ds(0, 1), cols]
    gb[...] = tall[...].astype(BF)
    go[...] = wide[...].astype(BF)
    for copy in copies:
        copy.wait()


def local(inputs, upstream, expand, biases, contract):
    vmem = pl.BlockSpec(memory_space=pltpu.VMEM)
    anywhere = pl.BlockSpec(memory_space=pl.ANY)
    dma = pltpu.SemaphoreType.DMA
    ox, oe, ob, oc, oo = pl.pallas_call(
        kernel,
        out_shape=(
            pltpu.VMEM((1024, 512), BF),
            pltpu.VMEM((512, 2048), BF),
            pltpu.VMEM((4, 8, 512), F32),
            pltpu.VMEM((2048, 512), BF),
            pltpu.VMEM((8, 512), F32),
        ),
        in_specs=[anywhere, anywhere, anywhere, vmem, anywhere],
        out_specs=(vmem, vmem, vmem, vmem, vmem),
        scratch_shapes=[
            pltpu.VMEM((4, 1024, 512), BF),
            pltpu.VMEM((4, 1024, 512), BF),
            pltpu.VMEM((4, 512, 512), BF),
            pltpu.VMEM((4, 512, 512), BF),
            pltpu.VMEM((2, 4, 2, 256, 256), F32),
            pltpu.VMEM((2, 4, 256, 256), F32),
            pltpu.VMEM((2, 2, 1024, 256), BF),
            pltpu.VMEM((2, 64, 512), BF),
            pltpu.VMEM((2, 64, 512), BF),
            pltpu.VMEM((4, 4, 128, 512), BF),
            pltpu.VMEM((4, 4, 128, 512), BF),
            pltpu.VMEM((2, 4, 4, 128, 512), BF),
            pltpu.VMEM((6, 2, 128, 512), BF),
            pltpu.VMEM((6, 2, 128, 512), BF),
            pltpu.VMEM((2, 6, 2, 128, 512), BF),
            pltpu.VMEM((4, 128, 512), BF),
            pltpu.VMEM((4, 128, 512), BF),
            pltpu.VMEM((2, 4, 128, 512), BF),
            pltpu.VMEM((2, 64, 512), BF),
            pltpu.VMEM((2, 64, 512), BF),
            pltpu.VMEM((2, 4, 64, 512), BF),
            pltpu.VMEM((2, 4, 64, 512), BF),
            pltpu.VMEM((2, 6, 32, 512), BF),
            pltpu.VMEM((16, 512), F32),
            pltpu.VMEM((3, 16, 512), F32),
            pltpu.VMEM((4, 256, 256), F32),
            dma((224,)),
            dma((224,)),
            dma((4,)),
            dma((2, 4)),
            dma((2, 4)),
            dma((2, 4)),
            dma((2, 4)),
        ],
        compiler_params=pltpu.CompilerParams(
            collective_id=0, has_side_effects=True, vmem_limit_bytes=50 * 1024 * 1024
        ),
    )(inputs, upstream, expand, biases.reshape(8, 1, 256), contract)
    gx, ge, gb, gc, go = pl.pallas_call(
        finish,
        out_shape=(
            jax.ShapeDtypeStruct((1024, 512), BF),
            jax.ShapeDtypeStruct((512, 2048), BF),
            jax.ShapeDtypeStruct((16, 128), BF),
            jax.ShapeDtypeStruct((2048, 512), BF),
            jax.ShapeDtypeStruct((4, 128), BF),
        ),
        in_specs=[vmem] * 5,
        out_specs=(anywhere, anywhere, vmem, anywhere, vmem),
        scratch_shapes=[pltpu.VMEM((16, 128), F32), pltpu.VMEM((4, 128), F32), dma((3,))],
        compiler_params=pltpu.CompilerParams(vmem_limit_bytes=12 * 1024 * 1024),
    )(ox, oe, ob, oc, oo)
    return gx, ge, gb.reshape(2048), gc, go.reshape(512)


def solution(mesh):
    in_specs = (P("dp", "row"), P("dp", "row"), P("row", "col"), P("col"), P("col", "row"))
    out_specs = (P("dp", "row"), P("row", "col"), P("col"), P("col", "row"), P("row"))
    return jax.shard_map(local, mesh=mesh, in_specs=in_specs, out_specs=out_specs, check_vma=False)
```

```python
import functools

import jax
import jax.numpy as jnp
from jax import lax
from jax.experimental import pallas as pl
from jax.experimental.pallas import tpu as pltpu
from jax.sharding import PartitionSpec as P

BF = jnp.bfloat16
F32 = jnp.float32
MESH = pl.DeviceIdType.MESH
NN = (((1,), (0,)), ((), ()))
NT = (((1,), (1,)), ((), ()))
TN = (((0,), (0,)), ((), ()))


def dot(a, b, dims):
    return lax.dot_general(a, b, dims, preferred_element_type=F32)


class Net:
    def __init__(self, send_sem, recv_sem):
        self.send_sem, self.recv_sem = send_sem, recv_sem
        self.used, self.sent = 0, []

    def ids(self, count):
        first = self.used
        self.used += count
        return range(first, first + count)

    def send(self, k, src, dst, device):
        copy = pltpu.make_async_remote_copy(
            src, dst, self.send_sem.at[k], self.recv_sem.at[k], device_id=device, device_id_type=MESH
        )
        copy.start()
        self.sent.append(copy)

    def arrived(self, k, dst, device):
        pltpu.make_async_remote_copy(
            dst, dst, self.send_sem.at[k], self.recv_sem.at[k], device_id=device, device_id_type=MESH
        ).wait_recv()

    def drain(self):
        for copy in self.sent:
            copy.wait_send()


class Gather:
    def __init__(self, net, me, left, right, full, top, bottom):
        self.net, self.me, self.left, self.right = net, me, left, right
        self.full, self.top, self.bottom = full, top, bottom
        self.k = net.ids(4)

    def start(self):
        block = self.full(self.me)
        self.net.send(self.k[0], block, block, self.right)
        self.net.send(self.k[1], block, block, self.left)

    def near(self):
        self.net.arrived(self.k[0], self.full((self.me + 3) % 4), self.left)
        self.net.arrived(self.k[1], self.full((self.me + 1) % 4), self.right)

    def forward(self):
        before, after = (self.me + 3) % 4, (self.me + 1) % 4
        self.net.arrived(self.k[0], self.full(before), self.left)
        self.net.send(self.k[2], self.top(before), self.top(before), self.right)
        self.net.arrived(self.k[1], self.full(after), self.right)
        self.net.send(self.k[3], self.bottom(after), self.bottom(after), self.left)

    def finish(self):
        across = (self.me + 2) % 4
        self.net.arrived(self.k[2], self.top(across), self.left)
        self.net.arrived(self.k[3], self.bottom(across), self.right)


class Exchange:
    def __init__(self, net, me, left, right, src, dst, relay, rows):
        self.net, self.me, self.left, self.right = net, me, left, right
        self.src, self.dst, self.relay, self.rows = src, dst, relay, rows
        self.k = net.ids(6)

    def start(self):
        me, half = self.me, self.rows // 2
        before, after, across = (me + 3) % 4, (me + 1) % 4, (me + 2) % 4
        self.net.send(self.k[2], self.src(across, 0, half), self.relay.at[0], self.right)
        self.net.send(self.k[3], self.src(across, half, half), self.relay.at[1], self.left)
        self.net.send(self.k[0], self.src(after, 0, self.rows), self.dst(me, 0, self.rows), self.right)
        self.net.send(self.k[1], self.src(before, 0, self.rows), self.dst(me, 0, self.rows), self.left)

    def forward(self):
        me, half = self.me, self.rows // 2
        before, after = (me + 3) % 4, (me + 1) % 4
        self.net.arrived(self.k[2], self.relay.at[0], self.left)
        self.net.send(self.k[4], self.relay.at[0], self.dst(before, 0, half), self.right)
        self.net.arrived(self.k[3], self.relay.at[1], self.right)
        self.net.send(self.k[5], self.relay.at[1], self.dst(after, half, half), self.left)

    def near(self):
        me = self.me
        self.net.arrived(self.k[0], self.dst((me + 3) % 4, 0, self.rows), self.left)
        self.net.arrived(self.k[1], self.dst((me + 1) % 4, 0, self.rows), self.right)

    def finish(self):
        half, across = self.rows // 2, (self.me + 2) % 4
        self.net.arrived(self.k[4], self.dst(across, 0, half), self.left)
        self.net.arrived(self.k[5], self.dst(across, half, half), self.right)


class Reduce:
    def __init__(self, net, me, left, right, part, inbox, add, total):
        self.net, self.me, self.left, self.right = net, me, left, right
        self.part, self.inbox, self.add, self.total = part, inbox, add, total
        self.k = net.ids(6)

    def far(self):
        across = (self.me + 2) % 4
        self.net.send(self.k[0], self.part(across, 0), self.inbox.at[0], self.right)
        self.net.send(self.k[1], self.part(across, 1), self.inbox.at[1], self.left)

    def near(self):
        before, after = (self.me + 3) % 4, (self.me + 1) % 4
        self.net.send(self.k[2], self.part(after, 1), self.inbox.at[2], self.right)
        self.net.send(self.k[3], self.part(before, 0), self.inbox.at[3], self.left)

    def join(self):
        before, after = (self.me + 3) % 4, (self.me + 1) % 4
        self.net.arrived(self.k[0], self.inbox.at[0], self.left)
        self.add(self.part(after, 0), self.inbox.at[0])
        self.net.send(self.k[4], self.part(after, 0), self.inbox.at[4], self.right)
        self.net.arrived(self.k[1], self.inbox.at[1], self.right)
        self.add(self.part(before, 1), self.inbox.at[1])
        self.net.send(self.k[5], self.part(before, 1), self.inbox.at[5], self.left)

    def finish(self):
        self.net.arrived(self.k[3], self.inbox.at[3], self.right)
        self.net.arrived(self.k[4], self.inbox.at[4], self.left)
        self.total(0, self.part(self.me, 0), self.inbox.at[3], self.inbox.at[4])
        self.net.arrived(self.k[2], self.inbox.at[2], self.left)
        self.net.arrived(self.k[5], self.inbox.at[5], self.right)
        self.total(1, self.part(self.me, 1), self.inbox.at[2], self.inbox.at[5])


def add_into(target, other):
    rows = min(128, target.shape[-2])
    lead = target.shape[0] if len(target.shape) == 3 else 1
    depth = target.shape[-2]

    def view(ref, i, r):
        where = pl.ds(pl.multiple_of(r * rows, rows), rows)
        return ref.at[i, where] if len(ref.shape) == 3 else ref.at[where]

    @pl.loop(0, lead * (depth // rows))
    def _(n):
        i, r = n // (depth // rows), n % (depth // rows)
        mine = view(target, i, r)
        mine[...] = (mine[...].astype(F32) + view(other, i, r)[...].astype(F32)).astype(BF)


def total_into(out, parts):
    rows = min(128, out.shape[-2])
    lead = out.shape[0] if len(out.shape) == 3 else 1
    depth = out.shape[-2]

    def view(ref, i, r):
        where = pl.ds(pl.multiple_of(r * rows, rows), rows)
        return ref.at[i, where] if len(ref.shape) == 3 else ref.at[where]

    @pl.loop(0, lead * (depth // rows))
    def _(n):
        i, r = n // (depth // rows), n % (depth // rows)
        acc = view(parts[0], i, r)[...].astype(F32)
        for other in parts[1:]:
            acc = acc + view(other, i, r)[...].astype(F32)
        view(out, i, r)[...] = acc.astype(BF)


def rows_at(start, size, unit):
    return pl.ds(pl.multiple_of(start, unit), size)


class PairRing:
    def __init__(self, net, zh, zl, outer, inner, block):
        self.net, self.outer, self.inner, self.block = net, outer, inner, block
        self.own, self.across = zh, (zh + 2) % 4
        self.early, self.late = (zh + 3 + 2 * zl) % 4, (zh + 5 - 2 * zl) % 4
        self.out_half, self.in_half = (1 - zl) * 128, zl * 128
        self.k = net.ids(4)

    def send(self, k, block, device):
        self.net.send(self.k[k], block, block, device)

    def start(self):
        self.send(0, self.block(self.own, 0, 256), self.outer)

    def get_early(self):
        block = self.block(self.early, 0, 256)
        self.net.arrived(self.k[0], block, self.outer)
        self.send(1, block, self.inner)

    def get_late(self):
        self.net.arrived(self.k[1], self.block(self.late, 0, 256), self.inner)
        self.send(2, self.block(self.late, self.out_half, 128), self.outer)

    def get_across(self):
        block = self.block(self.across, self.in_half, 128)
        self.net.arrived(self.k[2], block, self.outer)
        self.send(3, block, self.inner)

    def finish(self):
        self.net.arrived(self.k[3], self.block(self.across, self.out_half, 128), self.inner)


def kernel(
    x_ref, u_ref, e_ref, b_ref, c_ref,
    ox_ref, oe_ref, ob_ref, oc_ref, oo_ref,
    xg, ug, eg, cg, part, got, ah, relay_e, relay_c,
    ge, gc, gx, in_e, in_c, in_x, sum_e, sum_c, sum_x, relay_ge, relay_gc,
    pair_in, pair_sum, in_z, small, small_in, slope,
    send_sem, recv_sem, local_sem, hid_send, hid_recv, act_send, act_recv,
):
    row, col, x = lax.axis_index("row"), lax.axis_index("col"), lax.axis_index("dp")
    zh, c = row // 2, row % 2
    y, zl = col // 2, col % 2
    factor = 1.0 / 64.0

    z_right, z_left = {"row": ((zh + 1) % 4) * 2 + c}, {"row": ((zh + 3) % 4) * 2 + c}
    y_right, y_left = {"col": ((y + 1) % 4) * 2 + zl}, {"col": ((y + 3) % 4) * 2 + zl}
    x_right, x_left, x_across = {"dp": (x + 1) % 4}, {"dp": (x + 3) % 4}, {"dp": (x + 2) % 4}
    twin = {"row": zh * 2 + 1 - c}
    beside = {"col": y * 2 + 1 - zl}
    outer = {"row": ((zh + 3 + 2 * zl) % 4) * 2 + c, "col": y * 2 + 1 - zl}

    locals_ = [
        pltpu.make_async_copy(x_ref, xg.at[zh], local_sem.at[0]),
        pltpu.make_async_copy(u_ref, ug.at[zh], local_sem.at[1]),
        pltpu.make_async_copy(e_ref.at[:, rows_at(zh * 512, 512, 512)], eg.at[zh], local_sem.at[2]),
        pltpu.make_async_copy(c_ref.at[rows_at(zh * 512, 512, 512)], cg.at[zh], local_sem.at[3]),
    ]
    for copy in locals_:
        copy.start()

    barrier = pltpu.get_barrier_semaphore()
    peers = (z_right, z_left, y_right, y_left, x_right, x_left, x_across, twin, beside, outer)
    for peer in peers:
        pl.semaphore_signal(barrier, inc=1, device_id=peer, device_id_type=MESH)
    pl.semaphore_wait(barrier, len(peers))

    net = Net(send_sem, recv_sem)

    def z_gather(buf, slot):
        return PairRing(
            net, zh, zl, outer, beside, lambda j, first, size: buf.at[j, rows_at(slot * 256 + first, size, 128)]
        )

    def y_gathers(buf, ring):
        def gather(d):
            def at(size, first):
                return lambda j: buf.at[d, rows_at(j * 256 + first, size, 128)]
            return Gather(net, y, y_left, y_right, at(256, 0), at(128, 0), at(128, 128))
        return [gather(d) for d in (ring.early, ring.late, ring.across)]

    def x_gathers(at, order):
        return [
            Gather(net, x, x_left, x_right, at(d, 128, 0), at(d, 64, 0), at(d, 64, 64)) for d in order
        ]

    others = [(zh + d) % 4 for d in (3, 1, 2)]

    def weight_at(buf):
        return lambda d, size, first: lambda j: buf.at[d, rows_at(j * 128 + first, size, 64)]

    def weight_slot(buf):
        return lambda j, first, size: buf.at[j, rows_at(x * 128 + first, size, 64)]

    xz, uz = z_gather(xg, y), z_gather(ug, y)
    xy, uy = y_gathers(xg, xz), y_gathers(ug, uz)
    ez = Exchange(
        net, zh, z_left, z_right,
        lambda j, first, size: e_ref.at[rows_at(x * 128 + first, size, 64), rows_at(j * 512, 512, 512)],
        weight_slot(eg), relay_e, 128,
    )
    cz = Exchange(
        net, zh, z_left, z_right,
        lambda j, first, size: c_ref.at[rows_at(j * 512 + x * 128 + first, size, 64)],
        weight_slot(cg), relay_c, 128,
    )
    ex, cx = x_gathers(weight_at(eg), others), x_gathers(weight_at(cg), others)

    def hid_copy(k, slot):
        return pltpu.make_async_remote_copy(
            part.at[k, slot, 1 - c], got.at[k, slot], hid_send.at[k, slot], hid_recv.at[k, slot],
            device_id=twin, device_id_type=MESH,
        )

    def act_copy(k, slot, half):
        block = ah.at[k, half, rows_at(slot * 256, 256, 256)]
        return pltpu.make_async_remote_copy(
            block, block, act_send.at[k, slot], act_recv.at[k, slot],
            device_id=twin, device_id_type=MESH,
        )

    def forward_part(slot):
        where = rows_at(slot * 256, 256, 256)

        @pl.loop(0, 2)
        def _(half):
            cols = rows_at(half * 256, 256, 256)
            acc = dot(xg[0, where], eg[0, :, cols], NN)
            for j in range(1, 4):
                acc = acc + dot(xg[j, where], eg[j, :, cols], NN)
            part[0, slot, half] = acc

        hid_copy(0, slot).start()

    def back_half(half):
        cols = rows_at(half * 256, 256, 256)

        @pl.loop(0, 2)
        def _(n):
            where = rows_at(n * 512, 512, 512)
            acc = dot(ug[0, where], cg[0, cols], NT)
            for j in range(1, 4):
                acc = acc + dot(ug[j, where], cg[j, cols], NT)
            part[1, 2 * n, half] = acc[:256]
            part[1, 2 * n + 1, half] = acc[256:]

    def back_theirs():
        back_half(1 - c)

        @pl.loop(0, 4)
        def _(slot):
            hid_copy(1, slot).start()

    def activate(slot):
        hid_copy(0, slot).wait_recv()
        bias = b_ref[row]

        @pl.loop(0, 8)
        def _(r):
            rows = rows_at(r * 32, 32, 32)
            pre = part[0, slot, c, rows] + got[0, slot, rows] + bias
            v = pre.astype(BF).astype(F32)
            k0, k1 = 0.7978845608028654, 0.044715
            sq = v * v
            t = jnp.tanh(k0 * (v + k1 * (sq * v)))
            half = 0.5 * (1.0 + t)
            slope[slot, rows] = half + (0.5 * v) * (1.0 - t * t) * (k0 * (1.0 + 3.0 * k1 * sq))
            ah[0, c, rows_at(slot * 256 + r * 32, 32, 32)] = (v * half).astype(BF)

        act_copy(0, slot, c).start()

    def multiply(slot):
        hid_copy(1, slot).wait_recv()

        @pl.loop(0, 4)
        def _(r):
            rows = rows_at(r * 64, 64, 64)
            back = (part[1, slot, c, rows] + got[1, slot, rows]).astype(BF).astype(F32)
            ah[1, c, rows_at(slot * 256 + r * 64, 64, 64)] = (back * slope[slot, rows]).astype(BF)

        act_copy(1, slot, c).start()

    def swapped(k):
        @pl.loop(0, 4)
        def _(slot):
            act_copy(k, slot, 1 - c).wait_recv()
            hid_copy(k, slot).wait_send()
            act_copy(k, slot, c).wait_send()

    def reduce_to(axis, part_at, inbox, out):
        me, left, right = axis
        return Reduce(net, me, left, right, part_at, inbox, add_into,
                      lambda h, *parts: total_into(out(h), parts))

    over_x, over_y, over_z = (x, x_left, x_right), (y, y_left, y_right), (zh, z_left, z_right)
    e_red = reduce_to(over_x, lambda j, h: ge.at[j, pl.ds(2 * h, 2)], in_e, lambda h: sum_e.at[pl.ds(2 * h, 2)])
    c_red = reduce_to(over_x, lambda j, h: gc.at[j, pl.ds(2 * h, 2)], in_c, lambda h: sum_c.at[pl.ds(2 * h, 2)])

    def own_rows(s, first, size):
        return ox_ref.at[rows_at(y * 256 + s * 128 + zl * 64 + first, size, 32)]

    def per_chunk(s):
        down = reduce_to(over_y, lambda j, h: gx.at[s, j, pl.ds(2 * h, 2)], in_x.at[s],
                         lambda h: sum_x.at[s, pl.ds(2 * h, 2)])
        along = reduce_to(over_z, lambda j, h: pair_sum.at[s, j, pl.ds(32 * h, 32)], in_z.at[s],
                          lambda h: own_rows(s, 32 * h, 32))
        def at(size, first):
            return lambda j: ox_ref.at[rows_at(j * 256 + s * 128 + first, size, 64)]
        spread = Gather(net, y, y_left, y_right, at(128, 0), at(64, 0), at(64, 64))
        return down, along, spread, net.ids(2)

    chunks = [per_chunk(s) for s in range(2)]

    def out_e(j, first, size):
        return oe_ref.at[rows_at(x * 128 + first, size, 64), rows_at(j * 512, 512, 512)]

    def out_c(j, first, size):
        return oc_ref.at[rows_at(j * 512 + x * 128 + first, size, 64)]

    e_swap = Exchange(net, zh, z_left, z_right, lambda j, first, size: sum_e.at[j, pl.ds(first, size)],
                      out_e, relay_ge, 128)
    c_swap = Exchange(net, zh, z_left, z_right, lambda j, first, size: sum_c.at[j, pl.ds(first, size)],
                      out_c, relay_gc, 128)
    order = [zh] + others
    e_out = x_gathers(
        lambda d, size, first: lambda j: oe_ref.at[rows_at(j * 128 + first, size, 64), rows_at(d * 512, 512, 512)],
        order)
    c_out = x_gathers(
        lambda d, size, first: lambda j: oc_ref.at[rows_at(d * 512 + j * 128 + first, size, 64)], order)

    def pair_send(s):
        net.send(chunks[s][3][0], sum_x.at[s, :, rows_at((1 - zl) * 64, 64, 64)], pair_in.at[s], beside)

    def pair_add(s):
        net.arrived(chunks[s][3][0], pair_in.at[s], beside)

        @pl.loop(0, 4)
        def _(j):
            mine = sum_x[s, j, rows_at(zl * 64, 64, 64)].astype(F32)
            pair_sum[s, j] = (mine + pair_in[s, j].astype(F32)).astype(BF)

    def pair_back(s):
        net.send(chunks[s][3][1], own_rows(s, 0, 64), own_rows(s, 0, 64), beside)

    def pair_got(s):
        there = ox_ref.at[rows_at(y * 256 + s * 128 + (1 - zl) * 64, 64, 64)]
        net.arrived(chunks[s][3][1], there, beside)

    small_k = net.ids(6)

    def grad_expand():
        @pl.loop(0, 4)
        def _(j):
            for h in range(2):
                acc = (dot(xg[j], ah[1, h], TN) * factor).astype(BF)
                for q in range(4):
                    ge[q, j, :, pl.ds(h * 256, 256)] = acc[q * 128:(q + 1) * 128]

    def grad_contract(h):
        @pl.loop(0, 4)
        def _(j):
            acc = (dot(ah[0, h], ug[j], TN) * factor).astype(BF)
            gc[2 * h, j] = acc[:128]
            gc[2 * h + 1, j] = acc[128:]

    def grad_tokens(s):
        @pl.loop(0, 4)
        def _(j):
            first = ah[1, 0].reshape(4, 2, 128, 256)[:, s].reshape(512, 256)
            second = ah[1, 1].reshape(4, 2, 128, 256)[:, s].reshape(512, 256)
            acc = dot(first, eg[j, :, pl.ds(0, 256)], NT) + dot(second, eg[j, :, pl.ds(256, 256)], NT)
            acc = acc.astype(BF)
            for slot in range(4):
                gx[s, slot, j] = acc[slot * 128:(slot + 1) * 128]

    def token_sums():
        for h in range(2):
            def add_rows(n, acc):
                block = ah[1, h, rows_at(n * 64, 64, 64)].astype(F32)
                return acc + jnp.sum(block.reshape(8, 8, 256), axis=0)
            acc = lax.fori_loop(0, 16, add_rows, jnp.zeros((8, 256), F32))
            acc = jnp.sum(acc, axis=0, keepdims=True) * factor
            small[pl.ds(0, 8), pl.ds(h * 256, 256)] = jnp.broadcast_to(acc.astype(BF).astype(F32), (8, 256))

        def add_up(n, acc):
            block = ug[zh, rows_at(n * 64, 64, 64)].astype(F32)
            return acc + jnp.sum(block.reshape(8, 8, 512), axis=0)
        acc = lax.fori_loop(0, 16, add_up, jnp.zeros((8, 512), F32))
        acc = jnp.sum(acc, axis=0, keepdims=True) * factor
        small[pl.ds(8, 8)] = jnp.broadcast_to(acc.astype(BF).astype(F32), (8, 512))
        for n, peer in enumerate((x_right, x_left, x_across)):
            net.send(small_k[n], small, small_in.at[n], peer)

    def small_sums():
        for n, peer in enumerate((x_left, x_right, x_across)):
            net.arrived(small_k[n], small_in.at[n], peer)
        whole = ((small[...] + small_in[0]) + small_in[1]) + small_in[2]
        ob_ref[zh] = whole[:8]
        oo_ref[...] = whole[8:]
        for n, peer in enumerate((z_right, z_left)):
            net.send(small_k[3 + n], ob_ref.at[zh], ob_ref.at[zh], peer)

    def small_forward():
        before = ob_ref.at[(zh + 3) % 4]
        net.arrived(small_k[3], before, z_left)
        net.send(small_k[5], before, before, z_right)

    locals_[0].wait()
    xz.start()
    locals_[1].wait()
    uz.start()
    xz.get_early()
    xy[0].start()
    uz.get_early()
    uy[0].start()
    xy[0].forward()
    xz.get_late()
    xy[1].start()
    ez.start()
    xz.get_across()
    uz.get_late()
    uy[1].start()
    ez.near()
    ex[0].start()
    ex[1].start()
    ez.forward()
    xz.finish()
    xy[2].start()
    cz.start()
    ez.finish()
    ex[2].start()
    ex[0].forward()
    ex[1].forward()
    uy[1].forward()
    xy[2].forward()
    ex[2].forward()
    xy[1].forward()
    uz.get_across()
    cz.near()
    cx[0].start()
    cx[1].start()
    cz.forward()
    locals_[2].wait()
    for gather in ex:
        gather.finish()
    forward_part((y + 3) % 4)
    uz.finish()
    uy[2].start()
    forward_part((y + 1) % 4)
    uy[0].forward()
    forward_part(y)
    cz.finish()
    cx[2].start()
    activate(y)
    activate((y + 1) % 4)
    for gather in xy:
        gather.finish()
    forward_part((y + 2) % 4)
    activate((y + 3) % 4)
    cx[0].forward()
    cx[1].forward()
    uy[2].forward()
    activate((y + 2) % 4)
    cx[2].forward()
    swapped(0)
    for gather in uy:
        gather.finish()
    grad_contract((x + 2) % 4 // 2)
    c_red.far()
    locals_[3].wait()
    for gather in cx:
        gather.finish()
    back_theirs()
    back_half(c)
    multiply(y)
    grad_contract(1 - (x + 2) % 4 // 2)
    c_red.near()
    multiply((y + 3) % 4)
    multiply((y + 2) % 4)
    multiply((y + 1) % 4)
    swapped(1)
    grad_tokens(1)
    chunks[1][0].far()
    c_red.join()
    grad_expand()
    chunks[1][0].near()
    e_red.far()
    c_red.finish()
    oc_ref[rows_at(zh * 512 + x * 128, 128, 128)] = sum_c[zh]
    c_swap.start()
    chunks[1][0].join()
    e_red.near()
    grad_tokens(0)
    chunks[0][0].far()
    c_swap.forward()
    e_red.join()
    c_out[0].start()
    chunks[0][0].near()
    chunks[1][0].finish()
    pair_send(1)
    e_red.finish()
    oe_ref[rows_at(x * 128, 128, 128), rows_at(zh * 512, 512, 512)] = sum_e[zh]
    e_swap.start()
    chunks[0][0].join()
    c_swap.finish()
    c_out[3].start()
    pair_add(1)
    chunks[1][1].far()
    chunks[1][1].near()
    c_swap.near()
    c_out[1].start()
    c_out[2].start()
    chunks[0][0].finish()
    pair_send(0)
    c_out[0].forward()
    e_out[0].start()
    c_out[1].forward()
    token_sums()
    e_swap.near()
    e_out[1].start()
    e_out[2].start()
    e_out[0].forward()
    c_out[2].forward()
    chunks[1][1].join()
    pair_add(0)
    chunks[0][1].far()
    chunks[0][1].near()
    chunks[1][1].finish()
    pair_back(1)
    c_out[3].forward()
    chunks[0][1].join()
    e_out[1].forward()
    e_out[2].forward()
    e_swap.forward()
    pair_got(1)
    chunks[1][2].start()
    chunks[0][1].finish()
    pair_back(0)
    e_swap.finish()
    e_out[3].start()
    pair_got(0)
    chunks[0][2].start()
    small_sums()
    chunks[1][2].forward()
    small_forward()
    e_out[3].forward()
    chunks[0][2].forward()
    for gather in e_out + c_out:
        gather.finish()
    for chunk in chunks:
        chunk[2].finish()
    net.arrived(small_k[4], ob_ref.at[(zh + 1) % 4], z_right)
    net.arrived(small_k[5], ob_ref.at[(zh + 2) % 4], z_left)
    net.drain()
    assert net.used <= 224


def finish(ox, oe, ob, oc, oo, gx, ge, gb, gc, go, tall, wide, sem):
    copies = [
        pltpu.make_async_copy(src, dst, sem.at[k]) for k, (src, dst) in enumerate(((oe, ge), (oc, gc), (ox, gx)))
    ]
    for copy in copies:
        copy.start()
    for k in range(4):
        cols = pl.ds(k * 128, 128)
        for j in range(4):
            tall[pl.ds(j * 4 + k, 1)] = ob[j, pl.ds(0, 1), cols]
        wide[pl.ds(k, 1)] = oo[pl.ds(0, 1), cols]
    gb[...] = tall[...].astype(BF)
    go[...] = wide[...].astype(BF)
    for copy in copies:
        copy.wait()


def local(inputs, upstream, expand, biases, contract):
    vmem = pl.BlockSpec(memory_space=pltpu.VMEM)
    anywhere = pl.BlockSpec(memory_space=pl.ANY)
    dma = pltpu.SemaphoreType.DMA
    ox, oe, ob, oc, oo = pl.pallas_call(
        kernel,
        out_shape=(
            pltpu.VMEM((1024, 512), BF),
            pltpu.VMEM((512, 2048), BF),
            pltpu.VMEM((4, 8, 512), F32),
            pltpu.VMEM((2048, 512), BF),
            pltpu.VMEM((8, 512), F32),
        ),
        in_specs=[anywhere, anywhere, anywhere, vmem, anywhere],
        out_specs=(vmem, vmem, vmem, vmem, vmem),
        scratch_shapes=[
            pltpu.VMEM((4, 1024, 512), BF),
            pltpu.VMEM((4, 1024, 512), BF),
            pltpu.VMEM((4, 512, 512), BF),
            pltpu.VMEM((4, 512, 512), BF),
            pltpu.VMEM((2, 4, 2, 256, 256), F32),
            pltpu.VMEM((2, 4, 256, 256), F32),
            pltpu.VMEM((2, 2, 1024, 256), BF),
            pltpu.VMEM((2, 64, 512), BF),
            pltpu.VMEM((2, 64, 512), BF),
            pltpu.VMEM((4, 4, 128, 512), BF),
            pltpu.VMEM((4, 4, 128, 512), BF),
            pltpu.VMEM((2, 4, 4, 128, 512), BF),
            pltpu.VMEM((6, 2, 128, 512), BF),
            pltpu.VMEM((6, 2, 128, 512), BF),
            pltpu.VMEM((2, 6, 2, 128, 512), BF),
            pltpu.VMEM((4, 128, 512), BF),
            pltpu.VMEM((4, 128, 512), BF),
            pltpu.VMEM((2, 4, 128, 512), BF),
            pltpu.VMEM((2, 64, 512), BF),
            pltpu.VMEM((2, 64, 512), BF),
            pltpu.VMEM((2, 4, 64, 512), BF),
            pltpu.VMEM((2, 4, 64, 512), BF),
            pltpu.VMEM((2, 6, 32, 512), BF),
            pltpu.VMEM((16, 512), F32),
            pltpu.VMEM((3, 16, 512), F32),
            pltpu.VMEM((4, 256, 256), F32),
            dma((224,)),
            dma((224,)),
            dma((4,)),
            dma((2, 4)),
            dma((2, 4)),
            dma((2, 4)),
            dma((2, 4)),
        ],
        compiler_params=pltpu.CompilerParams(
            collective_id=0, has_side_effects=True, vmem_limit_bytes=50 * 1024 * 1024
        ),
    )(inputs, upstream, expand, biases.reshape(8, 1, 256), contract)
    gx, ge, gb, gc, go = pl.pallas_call(
        finish,
        out_shape=(
            jax.ShapeDtypeStruct((1024, 512), BF),
            jax.ShapeDtypeStruct((512, 2048), BF),
            jax.ShapeDtypeStruct((16, 128), BF),
            jax.ShapeDtypeStruct((2048, 512), BF),
            jax.ShapeDtypeStruct((4, 128), BF),
        ),
        in_specs=[vmem] * 5,
        out_specs=(anywhere, anywhere, vmem, anywhere, vmem),
        scratch_shapes=[pltpu.VMEM((16, 128), F32), pltpu.VMEM((4, 128), F32), dma((3,))],
        compiler_params=pltpu.CompilerParams(vmem_limit_bytes=12 * 1024 * 1024),
    )(ox, oe, ob, oc, oo)
    return gx, ge, gb.reshape(2048), gc, go.reshape(512)


def solution(mesh):
    in_specs = (P("dp", "row"), P("dp", "row"), P("row", "col"), P("col"), P("col", "row"))
    out_specs = (P("dp", "row"), P("row", "col"), P("col"), P("col", "row"), P("row"))
    return jax.shard_map(local, mesh=mesh, in_specs=in_specs, out_specs=out_specs, check_vma=False)
```
